32 devices in a mesh: ta: 4 (over y, x), gz: 2 (over core), xy: 4 (over z).
Axes of the slice: x: 2, y: 2, z: 4, core: 2. Of those that a mesh axis runs over, the one named last changes fastest.
Arguments:
- source_field: float32 [2, 4, 3, 4, 2, 4, 128], P(None, None, None, 'ta', 'gz', 'xy'), may hold values from -6 to 6
- gauge_links: float32 [2, 8, 3, 3, 4, 2, 4, 128], P(None, None, None, None, 'ta', 'gz', 'xy'), may hold values from -2.5 to 2.5
- fine_vectors: bfloat16 [2, 24, 4, 3, 4, 2, 4, 128], P(None, None, None, None, 'ta', 'gz', 'xy'), may hold values from -1.75 to 1.75
- middle_blocks: float32 [2, 9, 24, 4, 2, 4, 768], P(None, None, None, 'ta', 'gz', 'xy'), may hold values from -0.3125 to 0.3125
- middle_vectors: float32 [2, 24, 4, 2, 4, 768], P(None, None, 'ta', 'gz', 'xy'), may hold values from -0.625 to 0.625
- bottom_blocks: float32 [2, 7, 4, 2, 2304], P(None, None, 'ta', 'gz'), may hold values from -4 to 4
Outputs:
- solution: float32 [2, 4, 3, 4, 2, 4, 128], P(None, None, None, 'ta', 'gz', 'xy')
- smoothed_residual: float32 [2, 4, 3, 4, 2, 4, 128], P(None, None, None, 'ta', 'gz', 'xy')
The draws below stay inside these ranges and needn't reach their ends.
All inputs are finite; a program needn't handle non-finite values.
Results may differ from the reference program's by a relative error of at most 0.0034.
Values sent between devices are 32-bit elements; how exact they have to be, the bound alone decides.
No kernel may reach another device: no remote copies, remote signals or barrier semaphores. Data moves between devices by JAX's collectives and lax.ppermute only.
A program may use at most 64 MiB of HBM per device.

```python
import math
import jax
import jax.numpy as jnp
import numpy as np
from jax import lax

TL = 1
ZL = 1
XL = 1
YL = 128
BY = 4
NVEC = 24
NVEC2 = 24
YBLOCKS = 32
NT = 4
NZ = 2
NX = 4
N_TA = 4
N_GZ = 2
N_XY = 4


def draw_bottom_blocks(key, part):
    shape_list = (2, 7, NVEC2, NVEC2, N_TA, N_GZ, N_XY)
    entries = jax.random.normal(jax.random.fold_in(key, 11), shape_list, jnp.float32)
    spread = jnp.exp(jax.random.uniform(jax.random.fold_in(key, 13), (N_TA, N_GZ, N_XY), jnp.float32, -1.2, 1.2))
    rising = 3.0 ** (jnp.arange(N_TA, dtype=jnp.float32) / max(N_TA - 1, 1))
    scaling = spread * rising[:, None, None] / math.sqrt(14.0 * NVEC2)
    blocks = jnp.clip(entries * scaling, -4.0, 4.0)
    ordered = jnp.transpose(blocks, (0, 1, 4, 5, 6, 2, 3))
    return ordered.reshape((2, 7, N_TA, N_GZ, N_XY * NVEC2 * NVEC2))


def level_of(stream_key, dims, cuts, smallest, top_value):
    loudness, own = 1.0, jax.random.fold_in(stream_key, 6)
    for position, shards_of in cuts:
        draws = jnp.exp(jax.random.uniform(jax.random.fold_in(own, position), (shards_of,), jnp.float32, smallest / len(cuts), top_value / len(cuts)))
        loudness = loudness * jnp.repeat(draws, dims[position] // shards_of).reshape([-1 if axis == position else 1 for axis in range(len(dims))])
    return loudness


def bell_draw(own_key, dims, scale, limit, pieces=(), kind=jnp.bfloat16):
    level = level_of(own_key, dims, pieces, -0.22, 0.18) if pieces else 1.0
    drawn = jax.random.normal(own_key, dims, jnp.float32) * scale * level
    return jnp.minimum(jnp.maximum(drawn, -limit), limit).astype(kind)


def setup_inputs(seed: int = 0) -> dict:
    seeds = jax.random.split(jax.random.key(seed), 7)
    return {
        "source_field": bell_draw(seeds[0], (2, 4, 3, NT, NZ, NX, YL), 1.0, 6.0, ((3, 4), (4, 2), (5, 4)), jnp.float32),
        "gauge_links": bell_draw(seeds[1], (2, 8, 3, 3, NT, NZ, NX, YL), 6 ** -0.5, 2.5, ((4, 4), (5, 2), (6, 4)), jnp.float32),
        "fine_vectors": bell_draw(seeds[2], (2, NVEC, 4, 3, NT, NZ, NX, YL), (TL * ZL * XL * BY * 3) ** -0.5, 1.75, ((4, 4), (5, 2), (6, 4))),
        "middle_blocks": bell_draw(seeds[3], (2, 9, NVEC, N_TA, N_GZ, N_XY, NVEC * YBLOCKS), (18 * NVEC) ** -0.5, 0.3125, ((3, 4), (4, 2), (5, 4)), jnp.float32),
        "middle_vectors": bell_draw(seeds[4], (2, NVEC2, N_TA, N_GZ, N_XY, NVEC * YBLOCKS), (4 * NVEC) ** -0.5, 0.625, ((2, 4), (3, 2), (4, 4)), jnp.float32),
        "bottom_blocks": draw_bottom_blocks(jax.random.fold_in(seeds[6], 71), 0),
    }


quark_mass = 0.1
twist_mass = 0.1
fine_damping = 0.8
middle_damping = 0.4
middle_shift = 2.0
bottom_shift = 2.0

gamma_real = np.array([
    [[0, 0, 1, 0], [0, 0, 0, 1], [1, 0, 0, 0], [0, 1, 0, 0]],
    [[0] * 4] * 4,
    [[0] * 4] * 4,
    [[0, 0, 0, -1], [0, 0, 1, 0], [0, 1, 0, 0], [-1, 0, 0, 0]]], np.float32)
gamma_imag = np.array([
    [[0] * 4] * 4,
    [[0, 0, 1, 0], [0, 0, 0, -1], [-1, 0, 0, 0], [0, 1, 0, 0]],
    [[0, 0, 0, 1], [0, 0, 1, 0], [0, -1, 0, 0], [-1, 0, 0, 0]],
    [[0] * 4] * 4], np.float32)
chirality = np.array([1.0, 1.0, -1.0, -1.0], np.float32)


def color_apply(link_pair, spinor):
    link_re = link_pair[0][None]
    link_im = link_pair[1][None]
    part_re = spinor[0][:, None]
    part_im = spinor[1][:, None]
    real_part = jnp.sum(link_re * part_re - link_im * part_im, axis=2)
    imag_part = jnp.sum(link_re * part_im + link_im * part_re, axis=2)
    return jnp.stack([real_part, imag_part])


def apply_table(table_value, part_value):
    return jnp.tensordot(jnp.asarray(table_value), part_value, axes=([1], [0]), precision=lax.Precision.HIGHEST)


def spin_mix(spinor, direction):
    real_part = apply_table(gamma_real[direction], spinor[0]) - apply_table(gamma_imag[direction], spinor[1])
    imag_part = apply_table(gamma_real[direction], spinor[1]) + apply_table(gamma_imag[direction], spinor[0])
    return jnp.stack([real_part, imag_part])


def chirality_sign(spinor):
    return jnp.asarray(chirality).reshape((4,) + (1,) * (spinor.ndim - 2))


def twisted_diagonal(spinor):
    signs = chirality_sign(spinor)
    diagonal_value = 4.0 + quark_mass
    real_part = diagonal_value * spinor[0] - twist_mass * signs * spinor[1]
    imag_part = diagonal_value * spinor[1] + twist_mass * signs * spinor[0]
    return jnp.stack([real_part, imag_part])


def precondition(spinor):
    signs = chirality_sign(spinor)
    diagonal_value = 4.0 + quark_mass
    denominator = diagonal_value * diagonal_value + twist_mass * twist_mass
    real_part = (diagonal_value * spinor[0] + twist_mass * signs * spinor[1]) / denominator
    imag_part = (diagonal_value * spinor[1] - twist_mass * signs * spinor[0]) / denominator
    return jnp.stack([real_part, imag_part])


def wilson(spinor, ahead_list, behind_list, gauge_links):
    hopping = jnp.zeros_like(spinor)
    for direction in range(4):
        upward = color_apply(gauge_links[:, 2 * direction], ahead_list[direction])
        downward = color_apply(gauge_links[:, 2 * direction + 1], behind_list[direction])
        hopping = hopping + upward - spin_mix(upward, direction) + downward + spin_mix(downward, direction)
    return twisted_diagonal(spinor) - 0.5 * hopping


def fine_operator(spinor, gauge_links):
    ahead_list = [jnp.roll(spinor, -1, axis=3 + direction) for direction in range(4)]
    behind_list = [jnp.roll(spinor, 1, axis=3 + direction) for direction in range(4)]
    return wilson(spinor, ahead_list, behind_list, gauge_links)


def middle_layout(blocks):
    count = blocks.shape[2]
    split = blocks.reshape(blocks.shape[:6] + (count, blocks.shape[6] // count))
    return jnp.moveaxis(split, 6, 3)


def vector_layout(vectors):
    split = vectors.reshape(vectors.shape[:5] + (NVEC, vectors.shape[5] // NVEC))
    return jnp.moveaxis(split, 5, 2)


def bottom_layout(blocks):
    split = blocks.reshape(blocks.shape[:4] + (-1, NVEC2, NVEC2))
    return jnp.transpose(split, (0, 1, 5, 6, 2, 3, 4))


def block_apply(blocks, near_stack):
    def block_product(matrix, vector):
        return jnp.einsum('djk...,dk...->j...', matrix, vector, precision=lax.Precision.HIGHEST)
    real_part = block_product(blocks[0], near_stack[0]) - block_product(blocks[1], near_stack[1])
    imag_part = block_product(blocks[0], near_stack[1]) + block_product(blocks[1], near_stack[0])
    return jnp.stack([real_part, imag_part])


def restrict_middle(middle_vectors, coarse):
    def contract(left_side, right_side):
        return jnp.einsum('kjtzxa,jtzxa->ktzx', left_side, right_side, precision=lax.Precision.HIGHEST)
    real_part = contract(middle_vectors[0], coarse[0]) + contract(middle_vectors[1], coarse[1])
    imag_part = contract(middle_vectors[0], coarse[1]) - contract(middle_vectors[1], coarse[0])
    return jnp.stack([real_part, imag_part])


def prolong_middle(middle_vectors, coarse):
    def contract(left_side, right_side):
        return jnp.einsum('kjtzxa,ktzx->jtzxa', left_side, right_side, precision=lax.Precision.HIGHEST)
    real_part = contract(middle_vectors[0], coarse[0]) - contract(middle_vectors[1], coarse[1])
    imag_part = contract(middle_vectors[0], coarse[1]) + contract(middle_vectors[1], coarse[0])
    return jnp.stack([real_part, imag_part])


def inner_product(left_side, right_side):
    real_part = jnp.sum(left_side[0] * right_side[0] + left_side[1] * right_side[1])
    imag_part = jnp.sum(left_side[0] * right_side[1] - left_side[1] * right_side[0])
    return real_part, imag_part


def gram_partials(right_side, first_image, second_image):
    first_norm = inner_product(first_image, first_image)[0]
    second_norm = inner_product(second_image, second_image)[0]
    cross_re, cross_im = inner_product(first_image, second_image)
    first_re, first_im = inner_product(first_image, right_side)
    second_re, second_im = inner_product(second_image, right_side)
    return jnp.stack([first_norm, second_norm, cross_re, cross_im, first_re, first_im, second_re, second_im])


def complex_scale(coef_re, coef_im, vector):
    return jnp.stack([coef_re * vector[0] - coef_im * vector[1], coef_re * vector[1] + coef_im * vector[0]])


def least_squares(totals, right_side, first_image):
    first_norm = totals[0]
    second_norm = totals[1]
    cross_re = totals[2]
    cross_im = totals[3]
    first_re = totals[4]
    first_im = totals[5]
    second_re = totals[6]
    second_im = totals[7]
    determinant = first_norm * second_norm - cross_re * cross_re - cross_im * cross_im
    coef_one_re = (second_norm * first_re - (cross_re * second_re - cross_im * second_im)) / determinant
    coef_one_im = (second_norm * first_im - (cross_re * second_im + cross_im * second_re)) / determinant
    coef_two_re = (first_norm * second_re - (cross_re * first_re + cross_im * first_im)) / determinant
    coef_two_im = (first_norm * second_im - (cross_re * first_im - cross_im * first_re)) / determinant
    return complex_scale(coef_one_re, coef_one_im, right_side) + complex_scale(coef_two_re, coef_two_im, first_image)


def restrict_fine(residual_low, fine_vectors):
    split_vectors = fine_vectors.reshape((2, NVEC, 4, 3, N_TA, TL, N_GZ, ZL, N_XY, XL, YBLOCKS, BY))
    split_residual = residual_low.reshape((2, 4, 3, N_TA, TL, N_GZ, ZL, N_XY, XL, YBLOCKS, BY))
    collected = []
    for block in range(YBLOCKS):
        piece_vectors = split_vectors[..., block, :].astype(jnp.float32)
        piece_residual = split_residual[..., block, :].astype(jnp.float32)
        collected.append(jnp.einsum('pkscdefghib,qscdefghib->pqkdfh', piece_vectors, piece_residual,
                                    precision=lax.Precision.HIGHEST))
    terms = jnp.stack(collected, axis=-1)
    return jnp.stack([terms[0, 0] + terms[1, 1], terms[0, 1] - terms[1, 0]])


def prolong_fine(update_low, fine_vectors):
    split_vectors = fine_vectors.reshape((2, NVEC, 4, 3, N_TA, TL, N_GZ, ZL, N_XY, XL, YBLOCKS, BY))
    collected = []
    for block in range(YBLOCKS):
        piece_vectors = split_vectors[..., block, :].astype(jnp.float32)
        coefficients = update_low[..., block].astype(jnp.float32)
        terms = jnp.einsum('pkscdefghib,qkdfh->pqscdefghib', piece_vectors, coefficients,
                           precision=lax.Precision.HIGHEST)
        collected.append(jnp.stack([terms[0, 0] - terms[1, 1], terms[0, 1] + terms[1, 0]]))
    joined = jnp.stack(collected, axis=-2)
    return joined.reshape((2, 4, 3, NT, NZ, NX, YL))


def middle_operator(coarse, middle_blocks):
    near_list = [coarse]
    for axis_number in (2, 3, 4, 5):
        near_list.append(jnp.roll(coarse, -1, axis=axis_number))
        near_list.append(jnp.roll(coarse, 1, axis=axis_number))
    return middle_shift * coarse + block_apply(middle_blocks, jnp.stack(near_list, axis=1))


def bottom_operator(coarse, bottom_blocks):
    near_list = [coarse]
    for axis_number in (2, 3, 4):
        near_list.append(jnp.roll(coarse, -1, axis=axis_number))
        near_list.append(jnp.roll(coarse, 1, axis=axis_number))
    return bottom_shift * coarse + block_apply(bottom_blocks, jnp.stack(near_list, axis=1))


def reference(source_field, gauge_links, fine_vectors, middle_blocks, middle_vectors, bottom_blocks):
    middle_blocks = middle_layout(middle_blocks)
    middle_vectors = vector_layout(middle_vectors)
    bottom_blocks = bottom_layout(bottom_blocks)
    first_iterate = fine_damping * precondition(source_field)
    first_residual = source_field - fine_operator(first_iterate, gauge_links)
    second_iterate = first_iterate + fine_damping * precondition(first_residual)
    smoothed_residual = source_field - fine_operator(second_iterate, gauge_links)
    middle_right = restrict_fine(smoothed_residual.astype(jnp.bfloat16), fine_vectors)
    bottom_right = restrict_middle(middle_vectors, middle_right)
    first_image = bottom_operator(bottom_right, bottom_blocks)
    second_image = bottom_operator(first_image, bottom_blocks)
    totals = gram_partials(bottom_right, first_image, second_image)
    bottom_solution = least_squares(totals, bottom_right, first_image)
    middle_guess = prolong_middle(middle_vectors, bottom_solution)
    middle_update = middle_guess + middle_damping * (middle_right - middle_operator(middle_guess, middle_blocks))
    correction = prolong_fine(middle_update.astype(jnp.bfloat16), fine_vectors)
    return second_iterate + correction, smoothed_residual
```

```python
import functools
import math

import jax
import jax.numpy as jnp
import numpy as np
from jax import lax
from jax.experimental import pallas as pl
from jax.experimental.pallas import tpu as pltpu
from jax.sharding import PartitionSpec as P

BY = 4
NVEC = 24
NVEC2 = 24
SPINOR = 24
HALF = 12
LANES = 128
SUB = 8

quark_mass = 0.1
twist_mass = 0.1
fine_damping = 0.8
middle_damping = 0.4
middle_shift = 2.0
bottom_shift = 2.0
gamma = np.array(
    [
        [[0, 0, 1, 0], [0, 0, 0, 1], [1, 0, 0, 0], [0, 1, 0, 0]],
        [[0, 0, 1j, 0], [0, 0, 0, -1j], [-1j, 0, 0, 0], [0, 1j, 0, 0]],
        [[0, 0, 0, 1j], [0, 0, 1j, 0], [0, -1j, 0, 0], [-1j, 0, 0, 0]],
        [[0, 0, 0, -1], [0, 0, 1, 0], [0, 1, 0, 0], [-1, 0, 0, 0]],
    ],
    np.complex64,
)
chirality = np.array([1.0, 1.0, -1.0, -1.0])
HIGHEST = lax.Precision.HIGHEST
F32 = jnp.float32
BF16 = jnp.bfloat16


def real_form(matrix):
    return np.block([[matrix.real, -matrix.imag], [matrix.imag, matrix.real]])


def fine_tables():
    color = np.eye(3)
    project = np.zeros((2, 2, 3, 8, 8, SPINOR))
    rebuild = np.zeros((SPINOR, 2, 2, 3, 8))
    for m in range(4):
        for back in range(2):
            sign = -1.0 if back else 1.0
            way = 2 * m + back
            upper = np.eye(4)[:2] - sign * gamma[m][:2]
            project[:, :, :, way, way] = real_form(np.kron(upper, color)).reshape(2, 2, 3, SPINOR)
            lower = np.concatenate([np.eye(2), -sign * gamma[m][2:, :2]])
            rebuild[..., way] = real_form(np.kron(lower, color)).reshape(SPINOR, 2, 2, 3)
    project = project.reshape(HALF * 8, 8 * SPINOR)
    rebuild = rebuild.reshape(SPINOR, HALF * 8)
    mass = 4.0 + quark_mass
    twist = np.kron(np.diag(mass + 1j * twist_mass * chirality), color)
    diagonal = real_form(twist)
    inverse = real_form(np.linalg.inv(twist))
    first = project @ np.kron(np.eye(8), fine_damping * inverse)
    second = np.concatenate(
        [
            0.5 * fine_damping * inverse @ rebuild,
            fine_damping * (2.0 - fine_damping) * inverse,
        ],
        axis=1,
    )
    third = np.concatenate([0.5 * rebuild, -diagonal, np.eye(SPINOR)], axis=1)
    return [np.asarray(t, np.float32) for t in (first, second, project, third)]


def pairings(n):
    if n % 2:
        return [[((i + 1) % n, i) for i in range(n)], [(i, (i + 1) % n) for i in range(n)]]
    near = [(i, i ^ 1) for i in range(n)]
    far = [(i, (i + 1) % n if i % 2 else (i - 1) % n) for i in range(n)]
    return [near] if n == 2 else [near, far]


def neighbours(array, axes):
    found = []
    for axis in axes:
        pairs = pairings(lax.axis_size(axis))
        found.append([lax.ppermute(array, axis, p) for p in pairs])
    return found


def side_step(axis, which):
    n = lax.axis_size(axis)
    ahead = 1 if which == 0 else -1
    if n % 2:
        return ahead
    return ahead * (1 - 2 * (lax.axis_index(axis) % 2))


def ahead_behind(pair, axis):
    if len(pair) == 1:
        return pair[0], pair[0]
    n = lax.axis_size(axis)
    if n % 2:
        return pair[0], pair[1]
    even = lax.axis_index(axis) % 2 == 0
    return jnp.where(even, pair[0], pair[1]), jnp.where(even, pair[1], pair[0])


def dot(a, b):
    return jnp.dot(a, b, precision=HIGHEST, preferred_element_type=F32)


def dot_nt(a, b, precision=HIGHEST):
    return lax.dot_general(
        a, b, (((1,), (1,)), ((), ())), precision=precision, preferred_element_type=F32
    )


def parts(x):
    high = x.astype(BF16)
    rest = x - high.astype(F32)
    middle = rest.astype(BF16)
    low = (rest - middle.astype(F32)).astype(BF16)
    return high, middle, low


def iota(shape, dim):
    return lax.broadcasted_iota(jnp.int32, shape, dim)


def one_hot(condition, dtype=F32):
    return jnp.where(condition, 1.0, 0.0).astype(dtype)


def hopping(spinor, halos, gauge, project, axes):
    seen = []
    for pair, axis in zip(halos, axes):
        seen.extend(ahead_behind(pair, axis))
    seen.append(pltpu.roll(spinor, LANES - 1, 1))
    seen.append(pltpu.roll(spinor, 1, 1))
    half = dot(project, jnp.concatenate(seen, axis=0))
    rows = [[[None] * 3 for _ in range(2)] for _ in range(2)]
    for a in range(3):
        for b in range(3):
            link = [gauge[pl.ds(p * 72 + a * 3 + b, 8, stride=9), :] for p in range(2)]
            for s in range(2):
                re = half[(s * 3 + b) * 8 : (s * 3 + b) * 8 + 8]
                im = half[(6 + s * 3 + b) * 8 : (6 + s * 3 + b) * 8 + 8]
                out_re = link[0] * re - link[1] * im
                out_im = link[0] * im + link[1] * re
                for p, value in ((0, out_re), (1, out_im)):
                    old = rows[p][s][a]
                    rows[p][s][a] = value if old is None else old + value
    return [rows[p][s][a] for p in range(2) for s in range(2) for a in range(3)]


def first_kernel(counts, axes, *refs):
    source, refs = refs[0], refs[1:]
    halos, at = [], 0
    for count in counts:
        halos.append([r[...] for r in refs[at : at + count]])
        at += count
    gauge, vectors, project, table, out = refs[at:]
    value = source[...]
    rows = hopping(value, halos, gauge, project[...], axes)
    out[:SPINOR] = dot(table[...], jnp.concatenate(rows + [value], axis=0))
    out[SPINOR:] = vectors[...]


def strided_vectors(fine, i):
    row = (i % 3) * 4 + i // 3
    return [fine[pl.ds(p * NVEC * HALF + row, NVEC, stride=HALF), :] for p in range(2)]


def second_kernel(counts, axes, blocks, place, dests, *refs):
    source, own, refs = refs[0], refs[1], refs[2:]
    halos, at = [], 0
    for count in counts:
        halos.append([r[...] for r in refs[at : at + count]])
        at += count
    gauge, fine, vectors, project, table, out, middle, sent, wide = refs[at:]
    spinor = own[...]
    rows = hopping(spinor, halos, gauge, project[...], axes)
    residual = dot(table[...], jnp.concatenate(rows + [spinor, source[...]], axis=0))
    out[...] = residual
    low = residual.astype(BF16).astype(F32)
    wide[...] = fine[...].astype(F32)
    sum_re = jnp.zeros((NVEC, LANES), F32)
    sum_im = jnp.zeros((NVEC, LANES), F32)
    for i in range(HALF):
        re, im = strided_vectors(wide, i)
        low_re, low_im = low[i : i + 1], low[HALF + i : HALF + i + 1]
        sum_re = sum_re + re * low_re + im * low_im
        sum_im = sum_im + re * low_im - im * low_re
    group = iota((LANES, LANES), 1) % blocks == iota((LANES, LANES), 0) // BY
    right = dot(jnp.concatenate([sum_re, sum_im], axis=0), one_hot(group))
    middle[...] = right
    per = LANES // blocks
    count = NVEC // per
    keep = iota((NVEC, LANES), 1) // blocks == iota((NVEC, LANES), 0) % per
    pick = one_hot(iota((NVEC, NVEC), 1) // per == iota((NVEC, NVEC), 0) % count)
    kept = [jnp.where(keep, right[p * NVEC : (p + 1) * NVEC], 0.0) for p in range(2)]
    pattern = dot(pick, jnp.concatenate(kept, axis=1))
    pat_re, pat_im = pattern[:, :LANES], pattern[:, LANES:]
    size = NVEC2 * count
    made_re, made_im = [], []
    for block in range(size // NVEC):
        re = vectors[pl.ds(block * NVEC, NVEC), :]
        im = vectors[pl.ds(size + block * NVEC, NVEC), :]
        made_re.append(re * pat_re + im * pat_im)
        made_im.append(re * pat_im - im * pat_re)
    ones = jnp.ones((SUB, LANES), F32)
    shift = lax.axis_index("xy") * NVEC2 if place else 0
    scatter = one_hot(iota((size, LANES), 1) == iota((size, LANES), 0) // count + shift)
    line = [
        dot(dot_nt(ones, jnp.concatenate(made, axis=0)), scatter) for made in (made_re, made_im)
    ]
    both = jnp.where(iota((SUB, LANES), 0) % 2 == 0, line[0], line[1])
    for i in range(2 * dests // SUB):
        sent[i * SUB : (i + 1) * SUB] = both


def swap_pairs(x):
    return jnp.where(iota(x.shape, 0) % 2 == 0, pltpu.roll(x, SUB - 1, 0), pltpu.roll(x, 1, 0))


def bottom_apply(v, near, image, spread, gather, held, stride, nz, width):
    lane = iota(v.shape, 1)
    edge = width - NVEC2
    up = jnp.where(lane < edge, pltpu.roll(v, LANES - NVEC2, 1), pltpu.roll(v, edge, 1))
    down = jnp.where(lane >= NVEC2, pltpu.roll(v, NVEC2, 1), pltpu.roll(v, LANES - edge, 1))
    rows = jnp.concatenate([v, jnp.where(lane < width, up, 0.0), down], axis=0)
    total = None
    for part in parts(rows):
        term = jnp.dot(part, spread[...], preferred_element_type=F32)
        total = term if total is None else total + term
    near[...] = total
    chunks = near.shape[1] // LANES
    for c in range(chunks):
        here = pl.ds(c * LANES, LANES)
        own = [near[q * SUB : (q + 1) * SUB, here] for q in range(2)]
        side = [
            [near[(2 * d + q) * SUB : (2 * d + q + 1) * SUB, here] for q in range(2)]
            for d in (1, 2)
        ]
        stack = [
            (0, own),
            (1, [pltpu.roll(x, SUB - nz, 0) for x in own]),
            (2, [pltpu.roll(x, nz, 0) for x in own]),
            (3, [swap_pairs(x) for x in own]),
            (5, side[0]),
            (6, side[1]),
        ]
        acc_re = acc_im = None
        for d, (re, im) in stack:
            block = [held[pl.ds((p * 7 + d) * chunks + c, SUB, stride=stride), :] for p in range(2)]
            if d == 3:
                block = [
                    block[p] + held[pl.ds((p * 7 + 4) * chunks + c, SUB, stride=stride), :]
                    for p in range(2)
                ]
            got_re = block[0] * re - block[1] * im
            got_im = block[0] * im + block[1] * re
            acc_re = got_re if acc_re is None else acc_re + got_re
            acc_im = got_im if acc_im is None else acc_im + got_im
        image[:SUB, here] = acc_re
        image[SUB:, here] = acc_im
    total = bottom_shift * v
    for part in parts(image[...]):
        total = total + dot_nt(part, gather[...], None)
    return total


def whole_sum(x):
    return jnp.sum(jnp.sum(x, axis=1, keepdims=True), axis=0, keepdims=True)


def minimal_residual(r, f, s):
    r_re, r_im, f_re, f_im, s_re, s_im = r[:SUB], r[SUB:], f[:SUB], f[SUB:], s[:SUB], s[SUB:]
    ff = whole_sum(f_re * f_re + f_im * f_im)
    ss = whole_sum(s_re * s_re + s_im * s_im)
    cross_re = whole_sum(f_re * s_re + f_im * s_im)
    cross_im = whole_sum(f_re * s_im - f_im * s_re)
    one_re = whole_sum(f_re * r_re + f_im * r_im)
    one_im = whole_sum(f_re * r_im - f_im * r_re)
    two_re = whole_sum(s_re * r_re + s_im * r_im)
    two_im = whole_sum(s_re * r_im - s_im * r_re)
    determinant = ff * ss - cross_re * cross_re - cross_im * cross_im
    a_re = (ss * one_re - (cross_re * two_re - cross_im * two_im)) / determinant
    a_im = (ss * one_im - (cross_re * two_im + cross_im * two_re)) / determinant
    b_re = (ff * two_re - (cross_re * one_re + cross_im * one_im)) / determinant
    b_im = (ff * two_im - (cross_re * one_im - cross_im * one_re)) / determinant
    return jnp.concatenate(
        [
            a_re * r_re - a_im * r_im + b_re * f_re - b_im * f_im,
            a_re * r_im + a_im * r_re + b_re * f_im + b_im * f_re,
        ],
        axis=0,
    )


def bottom_rows(sites, shape, solution):
    nt, nz, nx = shape
    here = [lax.axis_index(a) for a in ("ta", "gz", "xy")]
    row, col = iota((2 * SUB, 2 * SUB), 0), iota((2 * SUB, 2 * SUB), 1)
    site = row // 2
    lines = jnp.full((2 * SUB, 2 * SUB), here[0] * nz + here[1], jnp.int32)
    turns = {0: [], 1: [], -1: []}
    at = 1
    side_rows = []
    for number, (axis, count) in enumerate(zip(("ta", "gz", "xy"), sites)):
        for which in range(count):
            step = side_step(axis, which)
            if number == 0:
                line = lax.rem(here[0] + step + nt, nt) * nz + here[1]
                lines = jnp.where(site == at, line, lines)
            elif number == 1:
                line = here[0] * nz + lax.rem(here[1] + step + nz, nz)
                lines = jnp.where(site == at, line, lines)
            else:
                side_rows.append((at, lax.rem(here[2] + step + nx, nx)))
            at += 1
    pick = one_hot((col % SUB == lines) & (col // SUB == row % 2))
    rows = dot(pick, solution)

    def turned(x):
        return pltpu.roll(rows, lax.rem(LANES - NVEC2 * x, LANES), 1)

    result = turned(here[2])
    for n, x in side_rows:
        result = jnp.where(iota(result.shape, 0) // 2 == n, turned(x), result)
    return jnp.where(iota(result.shape, 1) < NVEC2, result, 0.0)


def middle_step(counts, axes, blocks, rows, vectors, middle, read_block, fine, spinor, out, wide):
    per = LANES // blocks
    count = NVEC // per
    size = NVEC2 * count
    spread = one_hot(
        (iota((LANES, 2 * LANES), 0) == iota((LANES, 2 * LANES), 1) // count)
        & (iota((LANES, 2 * LANES), 1) < size),
        BF16,
    )
    coefs = None
    for part in parts(rows):
        term = jnp.dot(part, spread, preferred_element_type=F32)
        coefs = term if coefs is None else coefs + term
    same = iota((NVEC, size), 1) % count == iota((NVEC, size), 0) % count
    guesses = []
    for n, ref in enumerate(vectors):
        skip = ref.shape[0] - 2 * size
        wide_vectors = jnp.concatenate(
            [ref[skip : skip + size], ref[skip + size : skip + 2 * size]], axis=1
        )
        left = jnp.concatenate(
            [jnp.where(same, coefs[2 * n + q : 2 * n + q + 1, :size], 0.0) for q in range(2)],
            axis=0,
        )
        made = dot(left, wide_vectors)
        guesses.append(
            jnp.concatenate(
                [
                    made[:NVEC, :LANES] - made[NVEC:, LANES:],
                    made[:NVEC, LANES:] + made[NVEC:, :LANES],
                ],
                axis=0,
            )
        )
    own = guesses[0]
    near = [own]
    at = 1
    for c, axis in zip(counts, axes):
        near.extend(ahead_behind(guesses[at : at + c], axis))
        at += c
    aggregate = iota(own.shape, 1) % blocks
    near.append(
        jnp.where(
            aggregate == blocks - 1, pltpu.roll(own, blocks - 1, 1), pltpu.roll(own, LANES - 1, 1)
        )
    )
    near.append(
        jnp.where(aggregate == 0, pltpu.roll(own, LANES - blocks + 1, 1), pltpu.roll(own, 1, 1))
    )
    made_re, made_im = [], []
    for block in range(size // NVEC):
        acc_re = acc_im = None
        for d, value in enumerate(near):
            re, im = value[:NVEC], value[NVEC:]
            m_re, m_im = [read_block(p, d, block) for p in range(2)]
            got_re = m_re * re - m_im * im
            got_im = m_re * im + m_im * re
            acc_re = got_re if acc_re is None else acc_re + got_re
            acc_im = got_im if acc_im is None else acc_im + got_im
        row = iota((NVEC, LANES), 0) + block * NVEC
        at_home = (row % count) * per + iota((NVEC, LANES), 1) // blocks == row // count
        keep = 1.0 - middle_damping * middle_shift
        made_re.append(jnp.where(at_home, keep * own[:NVEC], 0.0) - middle_damping * acc_re)
        made_im.append(jnp.where(at_home, keep * own[NVEC:], 0.0) - middle_damping * acc_im)
    made = jnp.concatenate(
        [jnp.concatenate(made_re, axis=0), jnp.concatenate(made_im, axis=0)], axis=1
    )
    row_sum = one_hot(iota((NVEC, size), 1) // count == iota((NVEC, size), 0))
    summed = dot(row_sum, made)
    summed = jnp.concatenate([summed[:, :LANES], summed[:, LANES:]], axis=0)
    lane_sum = one_hot(
        iota((LANES, LANES), 0) % blocks == iota((LANES, LANES), 1) % blocks
    )
    update = dot(summed, lane_sum) + middle_damping * middle[...]
    lift = one_hot(iota((LANES, LANES), 0) == iota((LANES, LANES), 1) // BY, BF16)
    lifted = jnp.dot(update.astype(BF16), lift, preferred_element_type=F32)
    u_re, u_im = lifted[:NVEC], lifted[NVEC:]
    wide[...] = fine[...].astype(F32)
    sum_re, sum_im = [], []
    for i in range(HALF):
        re, im = strided_vectors(wide, i)
        sum_re.append(jnp.sum(re * u_re - im * u_im, axis=0, keepdims=True))
        sum_im.append(jnp.sum(re * u_im + im * u_re, axis=0, keepdims=True))
    out[...] = spinor[...] + jnp.concatenate(sum_re + sum_im, axis=0)


def third_kernel(counts, axes, blocks, shape, received, *refs):
    n_sites = 1 + sum(counts)
    held_in, refs = refs[:4], refs[4:]
    spread_in, gather_in, matrix_in, refs = refs[0], refs[1], refs[2], refs[3:]
    vectors, refs = refs[:n_sites], refs[n_sites:]
    middle, fine, spinor, out = refs[:4]
    held, spread, gather, matrix, near, image, wide, sems = refs[4:]
    nt, nz, nx = shape
    stride = held.shape[0] // SUB
    depth = held_in[0].shape[0] // 2
    ta, gz = lax.axis_index("ta"), lax.axis_index("gz")
    copies = []
    for i, ref in enumerate(held_in):
        for h in range(2):
            line = (ta ^ (2 * (i % 2) + h)) * nz + (gz ^ (i // 2))
            target = held.at[pl.ds(pl.multiple_of(line * stride, SUB), depth)]
            copies.append(
                pltpu.make_async_copy(ref.at[pl.ds(h * depth, depth)], target, sems.at[2 * i + h])
            )
    copies.append(pltpu.make_async_copy(spread_in, spread, sems.at[8]))
    copies.append(pltpu.make_async_copy(gather_in, gather, sems.at[9]))
    matrix_copy = pltpu.make_async_copy(matrix_in, matrix, sems.at[10])
    for copy in copies:
        copy.start()
    matrix_copy.start()
    total = received.shape[0]
    row, col = iota((2 * SUB, total), 0), iota((2 * SUB, total), 1)
    fold = one_hot((col // (2 * nx) == row % SUB) & (col % 2 == row // SUB))
    r = dot(fold, received[...])
    for copy in copies:
        copy.wait()
    apply = functools.partial(
        bottom_apply,
        near=near,
        image=image,
        spread=spread,
        gather=gather,
        held=held,
        stride=stride,
        nz=nz,
        width=nx * NVEC2,
    )
    f = apply(r)
    s = apply(f)
    rows = bottom_rows(counts, shape, minimal_residual(r, f, s))
    matrix_copy.wait()
    size = NVEC * NVEC * blocks // LANES

    def read_block(p, d, block):
        return matrix[pl.ds((p * 9 + d) * size + block * NVEC, NVEC), :]

    middle_step(
        counts, axes, blocks, rows, vectors, middle, read_block, fine, spinor, out, wide
    )


def fourth_kernel(counts, axes, blocks, rows, *refs):
    n_sites = 1 + sum(counts)
    matrix, refs = refs[0], refs[1:]
    vectors, refs = refs[:n_sites], refs[n_sites:]
    middle, fine, spinor, out, wide = refs
    size = NVEC * NVEC * blocks // LANES

    def read_block(p, d, block):
        return matrix[pl.ds((p * 9 + d) * size + block * NVEC, NVEC), :]

    middle_step(
        counts, axes, blocks, rows[...], vectors, middle, read_block, fine, spinor, out, wide
    )


def vmem():
    return pl.BlockSpec(memory_space=pltpu.VMEM)


def anywhere():
    return pl.BlockSpec(memory_space=pl.ANY)


def top(rows):
    return pl.BlockSpec((rows, LANES), lambda i: (0, 0))


def shape_of(*dims):
    return jax.ShapeDtypeStruct(dims, F32)


def params(mib):
    return pltpu.CompilerParams(vmem_limit_bytes=mib * 2**20)


def line_solve(right, bottom_blocks):
    split = bottom_blocks.reshape((2, 7, -1, NVEC2, NVEC2))
    line = lax.all_gather(right, "xy", axis=1, tiled=False)

    def moved(v, axis, step):
        n = lax.axis_size(axis)
        return lax.ppermute(v, axis, [((i + step) % n, i) for i in range(n)])

    def product(blocks, v):
        return jnp.einsum("dxjk,dxk->xj", blocks, v, precision=HIGHEST)

    def apply(v):
        near = [v, moved(v, "ta", 1), moved(v, "ta", -1), moved(v, "gz", 1), moved(v, "gz", -1)]
        near = jnp.stack(near + [jnp.roll(v, -1, 1), jnp.roll(v, 1, 1)], axis=1)
        re = product(split[0], near[0]) - product(split[1], near[1])
        im = product(split[0], near[1]) + product(split[1], near[0])
        return bottom_shift * v + jnp.stack([re, im])

    first = apply(line)
    second = apply(first)

    def inner(u, w):
        return [jnp.sum(u[0] * w[0] + u[1] * w[1]), jnp.sum(u[0] * w[1] - u[1] * w[0])]

    sums = inner(first, first)[:1] + inner(second, second)[:1] + inner(first, second)
    sums = sums + inner(first, line) + inner(second, line)
    ff, ss, cr, ci, pr, pi, qr, qi = lax.psum(jnp.stack(sums), ("ta", "gz"))
    det = ff * ss - cr * cr - ci * ci
    a_re = (ss * pr - (cr * qr - ci * qi)) / det
    a_im = (ss * pi - (cr * qi + ci * qr)) / det
    b_re = (ff * qr - (cr * pr + ci * pi)) / det
    b_im = (ff * qi - (cr * pi - ci * pr)) / det

    def scaled(re, im, v):
        return jnp.stack([re * v[0] - im * v[1], re * v[1] + im * v[0]])

    solved = scaled(a_re, a_im, line) + scaled(b_re, b_im, first)
    return lax.dynamic_index_in_dim(solved, lax.axis_index("xy"), 1, keepdims=False)


def shards(source_field, gauge_links, fine_vectors, middle_blocks, middle_vectors, bottom_blocks):
    axes = ("ta", "gz", "xy")
    shape = tuple(lax.axis_size(a) for a in axes)
    nt, nz, nx = shape
    devices = nt * nz * nx
    blocks = source_field.shape[-1] // BY
    source = source_field.reshape(SPINOR, LANES)
    gauge = gauge_links.reshape(-1, LANES)
    fine = jnp.transpose(fine_vectors, (0, 1, 3, 4, 5, 6, 2, 7)).reshape(-1, LANES)
    matrix = middle_blocks.reshape(-1, LANES)
    vectors = middle_vectors.reshape(-1, LANES)
    size = vectors.shape[0]
    first, second, project, third = fine_tables()
    counts = [len(pairings(n)) for n in shape]
    gathered = nt == 4 and nz == 2 and nx * NVEC2 <= LANES

    halos = neighbours(source, axes)
    flat = [a for pair in halos for a in pair]
    if gathered:
        per_line = bottom_blocks.shape[-1] * 14 // LANES
        depth = -(-per_line // SUB) * SUB
        line = jnp.pad(bottom_blocks.reshape(per_line, LANES), ((0, depth - per_line), (0, 0)))
        pair = jnp.concatenate([line, lax.ppermute(line, "ta", [(i, i ^ 1) for i in range(nt)])])
    payload = pl.pallas_call(
        functools.partial(first_kernel, counts, axes),
        out_shape=shape_of(SPINOR + size, LANES),
        in_specs=[vmem()] * (len(flat) + 5),
        out_specs=vmem(),
        compiler_params=params(8),
    )(source, *flat, gauge, vectors, first, second)

    near = neighbours(payload, axes)
    flat_near = [a for pair in near for a in pair]
    if gathered:
        other = lax.ppermute(pair, "ta", [(i, i ^ 2) for i in range(nt)])
        swap = [(i, i ^ 1) for i in range(nz)]
        held = [pair, other, lax.ppermute(pair, "gz", swap), lax.ppermute(other, "gz", swap)]
    dests = devices if gathered else SUB
    residual, middle, sent = pl.pallas_call(
        functools.partial(second_kernel, counts, axes, blocks, gathered, dests),
        out_shape=(
            shape_of(SPINOR, LANES),
            shape_of(2 * NVEC, LANES),
            shape_of(2 * dests, LANES),
        ),
        grid=(1,),
        in_specs=[vmem()] + [top(SPINOR)] * (1 + len(flat_near)) + [vmem()] * 5,
        out_specs=(vmem(), vmem(), vmem()),
        scratch_shapes=[pltpu.VMEM(fine.shape, F32)],
        compiler_params=params(8),
    )(source, payload, *flat_near, gauge, fine, vectors, project, third)

    if gathered:
        received = lax.all_to_all(sent.reshape(devices, 2, LANES), axes, 0, 0)
        received = received.reshape(2 * devices, LANES)
        lane = np.arange(nx * NVEC2 * NVEC2)
        k_lane = np.arange(LANES)[:, None]
        spread = k_lane == (lane // (NVEC2 * NVEC2) * NVEC2 + lane % NVEC2)[None]
        gather = k_lane == (lane // NVEC2)[None]
        spread, gather = jnp.asarray(spread, BF16), jnp.asarray(gather, BF16)
        wide = lane.size
        stride = depth + SUB
        solution = pl.pallas_call(
            functools.partial(third_kernel, counts, axes, blocks, shape),
            out_shape=shape_of(SPINOR, LANES),
            grid=(1,),
            in_specs=[vmem()]
            + [anywhere()] * 7
            + [vmem()] * (1 + len(flat_near))
            + [vmem(), vmem(), top(SPINOR)],
            out_specs=vmem(),
            scratch_shapes=[
                pltpu.VMEM((SUB * stride, LANES), F32),
                pltpu.VMEM(spread.shape, BF16),
                pltpu.VMEM(gather.shape, BF16),
                pltpu.VMEM(matrix.shape, F32),
                pltpu.VMEM((6 * SUB, wide), F32),
                pltpu.VMEM((2 * SUB, wide), F32),
                pltpu.VMEM(fine.shape, F32),
                pltpu.SemaphoreType.DMA((11,)),
            ],
            compiler_params=params(20),
        )(received, *held, spread, gather, matrix, vectors, *flat_near, middle, fine, payload)
    else:
        solved = line_solve(sent[:2, :NVEC2], bottom_blocks)
        solved = jnp.pad(solved, ((0, 0), (0, LANES - NVEC2)))
        rows = [solved] + [a for pair in neighbours(solved, axes) for a in pair]
        rows = jnp.concatenate(rows)
        rows = jnp.pad(rows, ((0, 2 * SUB - rows.shape[0]), (0, 0)))
        solution = pl.pallas_call(
            functools.partial(fourth_kernel, counts, axes, blocks),
            out_shape=shape_of(SPINOR, LANES),
            grid=(1,),
            in_specs=[vmem()] * (3 + len(flat_near)) + [vmem(), vmem(), top(SPINOR)],
            out_specs=vmem(),
            scratch_shapes=[pltpu.VMEM(fine.shape, F32)],
            compiler_params=params(16),
        )(rows, matrix, vectors, *flat_near, middle, fine, payload)
    return solution.reshape(source_field.shape), residual.reshape(source_field.shape)


def solution(mesh):
    return jax.shard_map(
        shards,
        mesh=mesh,
        in_specs=(
            P(None, None, None, "ta", "gz", "xy", None),
            P(None, None, None, None, "ta", "gz", "xy", None),
            P(None, None, None, None, "ta", "gz", "xy", None),
            P(None, None, None, "ta", "gz", "xy", None),
            P(None, None, "ta", "gz", "xy", None),
            P(None, None, "ta", "gz", None),
        ),
        out_specs=(
            P(None, None, None, "ta", "gz", "xy", None),
            P(None, None, None, "ta", "gz", "xy", None),
        ),
        check_vma=False,
    )
```

```python
import functools

import jax
import jax.numpy as jnp
import numpy as np
from jax import lax
from jax.experimental import pallas as pl
from jax.experimental.pallas import tpu as pltpu
from jax.sharding import PartitionSpec as P


BY = 4
NVEC = 24
NVEC2 = 24
SPINOR = 24
HALF = 12
LANES = 128
SUB = 8

quark_mass = 0.1
twist_mass = 0.1
fine_damping = 0.8
middle_damping = 0.4
middle_shift = 2.0
bottom_shift = 2.0
gamma = np.array(
    [
        [[0, 0, 1, 0], [0, 0, 0, 1], [1, 0, 0, 0], [0, 1, 0, 0]],
        [[0, 0, 1j, 0], [0, 0, 0, -1j], [-1j, 0, 0, 0], [0, 1j, 0, 0]],
        [[0, 0, 0, 1j], [0, 0, 1j, 0], [0, -1j, 0, 0], [-1j, 0, 0, 0]],
        [[0, 0, 0, -1], [0, 0, 1, 0], [0, 1, 0, 0], [-1, 0, 0, 0]],
    ],
    np.complex64,
)
chirality = np.array([1.0, 1.0, -1.0, -1.0])
HIGHEST = lax.Precision.HIGHEST
F32 = jnp.float32
BF16 = jnp.bfloat16


def real_form(matrix):
    return np.block([[matrix.real, -matrix.imag], [matrix.imag, matrix.real]])


def fine_tables():
    color = np.eye(3)
    project = np.zeros((2, 2, 3, 8, 8, SPINOR))
    rebuild = np.zeros((SPINOR, 2, 2, 3, 8))
    for m in range(4):
        for back in range(2):
            sign = -1.0 if back else 1.0
            way = 2 * m + back
            upper = np.eye(4)[:2] - sign * gamma[m][:2]
            project[:, :, :, way, way] = real_form(np.kron(upper, color)).reshape(2, 2, 3, SPINOR)
            lower = np.concatenate([np.eye(2), -sign * gamma[m][2:, :2]])
            rebuild[..., way] = real_form(np.kron(lower, color)).reshape(SPINOR, 2, 2, 3)
    project = project.reshape(HALF * 8, 8 * SPINOR)
    rebuild = rebuild.reshape(SPINOR, HALF * 8)
    mass = 4.0 + quark_mass
    twist = np.kron(np.diag(mass + 1j * twist_mass * chirality), color)
    diagonal = real_form(twist)
    inverse = real_form(np.linalg.inv(twist))
    first = project @ np.kron(np.eye(8), fine_damping * inverse)
    second = np.concatenate(
        [
            0.5 * fine_damping * inverse @ rebuild,
            fine_damping * (2.0 - fine_damping) * inverse,
        ],
        axis=1,
    )
    third = np.concatenate([0.5 * rebuild, -diagonal, np.eye(SPINOR)], axis=1)
    return [np.asarray(t, np.float32) for t in (first, second, project, third)]


def pairings(n):
    if n % 2:
        return [[((i + 1) % n, i) for i in range(n)], [(i, (i + 1) % n) for i in range(n)]]
    near = [(i, i ^ 1) for i in range(n)]
    far = [(i, (i + 1) % n if i % 2 else (i - 1) % n) for i in range(n)]
    return [near] if n == 2 else [near, far]


def neighbours(array, axes):
    found = []
    for axis in axes:
        pairs = pairings(lax.axis_size(axis))
        found.append([lax.ppermute(array, axis, p) for p in pairs])
    return found


def load_kernel(has_line, *refs):
    sems = refs[-1]
    count = sems.shape[0]
    ins, outs = refs[:count], list(refs[count : 2 * count])
    if has_line:
        out, outs[-1] = outs[-1], refs[-2]
    copies = [pltpu.make_async_copy(ins[i], outs[i], sems.at[i]) for i in range(count)]
    for copy in reversed(copies):
        copy.start()
    if has_line:
        copies[-1].wait()
        source = outs[-1]
        chunks = out.shape[0] // 12
        even = lax.axis_index("ta") % 2 == 0
        for p in range(2):
            way = [
                source[:, (p * 7 + d) * chunks * LANES : (p * 7 + d + 1) * chunks * LANES]
                for d in range(7)
            ]
            ahead, behind = way[1], way[2]
            ways = [way[0], jnp.where(even, ahead, behind), jnp.where(even, behind, ahead)]
            ways += [way[3] + way[4], way[5], way[6]]
            for d, value in enumerate(ways):
                for c in range(chunks):
                    row = (p * 6 + d) * chunks + c
                    out[row : row + 1] = value[:, c * LANES : (c + 1) * LANES]
        copies = copies[:-1]
    for copy in copies:
        copy.wait()


def side_step(axis, which):
    n = lax.axis_size(axis)
    ahead = 1 if which == 0 else -1
    if n % 2:
        return ahead
    return ahead * (1 - 2 * (lax.axis_index(axis) % 2))


def ahead_behind(pair, axis):
    if len(pair) == 1:
        return pair[0], pair[0]
    n = lax.axis_size(axis)
    if n % 2:
        return pair[0], pair[1]
    even = lax.axis_index(axis) % 2 == 0
    return jnp.where(even, pair[0], pair[1]), jnp.where(even, pair[1], pair[0])


def dot(a, b):
    return jnp.dot(a, b, precision=HIGHEST, preferred_element_type=F32)


def dot_nt(a, b, precision=HIGHEST):
    return lax.dot_general(
        a, b, (((1,), (1,)), ((), ())), precision=precision, preferred_element_type=F32
    )


def parts(x):
    high = x.astype(BF16)
    rest = x - high.astype(F32)
    middle = rest.astype(BF16)
    low = (rest - middle.astype(F32)).astype(BF16)
    return high, middle, low


def iota(shape, dim):
    return lax.broadcasted_iota(jnp.int32, shape, dim)


def one_hot(condition, dtype=F32):
    return jnp.where(condition, 1.0, 0.0).astype(dtype)


def hopping(spinor, halos, gauge, project, axes):
    seen = []
    for pair, axis in zip(halos, axes):
        seen.extend(ahead_behind(pair, axis))
    seen.append(pltpu.roll(spinor, LANES - 1, 1))
    seen.append(pltpu.roll(spinor, 1, 1))
    half = dot(project, jnp.concatenate(seen, axis=0))
    rows = [[[None] * 3 for _ in range(2)] for _ in range(2)]
    for a in range(3):
        for b in range(3):
            link = [gauge[pl.ds(p * 72 + a * 3 + b, 8, stride=9), :] for p in range(2)]
            for s in range(2):
                re = half[(s * 3 + b) * 8 : (s * 3 + b) * 8 + 8]
                im = half[(6 + s * 3 + b) * 8 : (6 + s * 3 + b) * 8 + 8]
                out_re = link[0] * re - link[1] * im
                out_im = link[0] * im + link[1] * re
                for p, value in ((0, out_re), (1, out_im)):
                    old = rows[p][s][a]
                    rows[p][s][a] = value if old is None else old + value
    return [rows[p][s][a] for p in range(2) for s in range(2) for a in range(3)]


def first_kernel(counts, axes, *refs):
    source, refs = refs[0], refs[1:]
    halos, at = [], 0
    for count in counts:
        halos.append([r[...] for r in refs[at : at + count]])
        at += count
    gauge, vectors, project, table, out = refs[at:]
    value = source[...]
    rows = hopping(value, halos, gauge, project[...], axes)
    out[:SPINOR] = dot(table[...], jnp.concatenate(rows + [value], axis=0))
    out[SPINOR:] = vectors[...]


def strided_vectors(fine, i):
    row = (i % 3) * 4 + i // 3
    return [fine[pl.ds(p * NVEC * HALF + row, NVEC, stride=HALF), :] for p in range(2)]


def second_kernel(counts, axes, blocks, place, dests, *refs):
    source, own, refs = refs[0], refs[1], refs[2:]
    halos, at = [], 0
    for count in counts:
        halos.append([r[...] for r in refs[at : at + count]])
        at += count
    gauge, fine, vectors, project, table, out, middle, sent, wide = refs[at:]
    spinor = own[...]
    rows = hopping(spinor, halos, gauge, project[...], axes)
    residual = dot(table[...], jnp.concatenate(rows + [spinor, source[...]], axis=0))
    out[...] = residual
    low = residual.astype(BF16).astype(F32)
    wide[...] = fine[...].astype(F32)
    sum_re = jnp.zeros((NVEC, LANES), F32)
    sum_im = jnp.zeros((NVEC, LANES), F32)
    for i in range(HALF):
        re, im = strided_vectors(wide, i)
        low_re, low_im = low[i : i + 1], low[HALF + i : HALF + i + 1]
        sum_re = sum_re + re * low_re + im * low_im
        sum_im = sum_im + re * low_im - im * low_re
    group = iota((LANES, LANES), 1) % blocks == iota((LANES, LANES), 0) // BY
    right = dot(jnp.concatenate([sum_re, sum_im], axis=0), one_hot(group))
    middle[...] = right
    per = LANES // blocks
    count = NVEC // per
    keep = iota((NVEC, LANES), 1) // blocks == iota((NVEC, LANES), 0) % per
    pick = one_hot(iota((NVEC, NVEC), 1) // per == iota((NVEC, NVEC), 0) % count)
    kept = [jnp.where(keep, right[p * NVEC : (p + 1) * NVEC], 0.0) for p in range(2)]
    pattern = dot(pick, jnp.concatenate(kept, axis=1))
    pat_re, pat_im = pattern[:, :LANES], pattern[:, LANES:]
    size = NVEC2 * count
    made_re, made_im = [], []
    for block in range(size // NVEC):
        re = vectors[pl.ds(block * NVEC, NVEC), :]
        im = vectors[pl.ds(size + block * NVEC, NVEC), :]
        made_re.append(re * pat_re + im * pat_im)
        made_im.append(re * pat_im - im * pat_re)
    ones = jnp.ones((SUB, LANES), F32)
    shift = lax.axis_index("xy") * NVEC2 if place else 0
    scatter = one_hot(iota((size, LANES), 1) == iota((size, LANES), 0) // count + shift)
    line = [
        dot(dot_nt(ones, jnp.concatenate(made, axis=0)), scatter) for made in (made_re, made_im)
    ]
    both = jnp.where(iota((SUB, LANES), 0) % 2 == 0, line[0], line[1])
    for i in range(2 * dests // SUB):
        sent[i * SUB : (i + 1) * SUB] = both


def exchanged(x, step):
    rows = x.shape[0]
    if rows == 2 * step:
        return pltpu.roll(x, step, 0)
    up, down = pltpu.roll(x, rows - step, 0), pltpu.roll(x, step, 0)
    return jnp.where(iota(x.shape, 0) // step % 2 == 0, up, down)


def bottom_apply(v, near, image, spread, gather, held, width):
    lane = iota(v.shape, 1)
    edge = width - NVEC2
    up = jnp.where(lane < edge, pltpu.roll(v, LANES - NVEC2, 1), pltpu.roll(v, edge, 1))
    down = jnp.where(lane >= NVEC2, pltpu.roll(v, NVEC2, 1), pltpu.roll(v, LANES - edge, 1))
    rows = jnp.concatenate([v, jnp.where(lane < width, up, 0.0), down], axis=0)
    total = None
    for part in parts(rows):
        term = jnp.dot(part, spread[...], preferred_element_type=F32)
        total = term if total is None else total + term
    near[...] = total
    chunks = near.shape[1] // LANES
    stride = 6 * chunks
    for c in range(chunks):
        here = pl.ds(c * LANES, LANES)
        seen = [near[i * SUB : (i + 1) * SUB, here] for i in range(6)]
        turned = [exchanged(x, 1) for x in seen]
        for core in range(2):
            acc = [None, None]
            for n, rows in enumerate((seen, turned)):
                beside = exchanged(rows[core], 2)
                ways = [rows[core], beside, pltpu.roll(beside, 4, 0), rows[1 - core]]
                ways += [rows[2 + core], rows[4 + core]]
                for d, value in enumerate(ways):
                    block = held[core][pl.ds(d * chunks + c, SUB, stride=stride), :]
                    got = block * value
                    acc[n] = got if acc[n] is None else acc[n] + got
                image[(2 * n + core) * SUB : (2 * n + core + 1) * SUB, here] = acc[n]
    total = None
    for part in parts(image[...]):
        term = dot_nt(part, gather[...], None)
        total = term if total is None else total + term
    first, second = total[: 2 * SUB], total[2 * SUB :]
    re = first - exchanged(first, 1)
    im = second + exchanged(second, 1)
    return bottom_shift * v + jnp.where(iota(v.shape, 0) % 2 == 0, re, im)


def whole_sum(x):
    return jnp.sum(jnp.sum(x, axis=1, keepdims=True), axis=0, keepdims=True)


def minimal_residual(r, f, s):
    sign = jnp.where(iota(r.shape, 0) % 2 == 0, 1.0, -1.0)
    r_turn, s_turn, f_turn = exchanged(r, 1), exchanged(s, 1), exchanged(f, 1)
    ff = whole_sum(f * f)
    ss = whole_sum(s * s)
    cross_re = whole_sum(f * s)
    cross_im = whole_sum(sign * f * s_turn)
    one_re = whole_sum(f * r)
    one_im = whole_sum(sign * f * r_turn)
    two_re = whole_sum(s * r)
    two_im = whole_sum(sign * s * r_turn)
    determinant = ff * ss - cross_re * cross_re - cross_im * cross_im
    a_re = (ss * one_re - (cross_re * two_re - cross_im * two_im)) / determinant
    a_im = (ss * one_im - (cross_re * two_im + cross_im * two_re)) / determinant
    b_re = (ff * two_re - (cross_re * one_re + cross_im * one_im)) / determinant
    b_im = (ff * two_im - (cross_re * one_im - cross_im * one_re)) / determinant
    return a_re * r + b_re * f - sign * (a_im * r_turn + b_im * f_turn)


def bottom_rows(nx, solution):
    rows = jnp.concatenate(
        [
            solution[0:4],
            solution[6:10],
            solution[0:2],
            solution[0:2],
            jnp.zeros((4, LANES), F32),
        ],
        axis=0,
    )
    x = lax.axis_index("xy")

    def turned(step):
        place = lax.rem(x + step + nx, nx)
        return pltpu.roll(rows, lax.rem(LANES - NVEC2 * place, LANES), 1)

    site = iota(rows.shape, 0) // 2
    near, far = turned(side_step("xy", 0)), turned(side_step("xy", 1))
    result = jnp.where(site == 4, near, jnp.where(site == 5, far, turned(0)))
    return jnp.where(iota(result.shape, 1) < NVEC2, result, 0.0)


def middle_step(counts, axes, blocks, rows, vectors, middle, read_block, fine, spinor, out, wide):
    per = LANES // blocks
    count = NVEC // per
    size = NVEC2 * count
    spread = one_hot(
        (iota((LANES, 2 * LANES), 0) == iota((LANES, 2 * LANES), 1) // count)
        & (iota((LANES, 2 * LANES), 1) < size),
        BF16,
    )
    coefs = None
    for part in parts(rows):
        term = jnp.dot(part, spread, preferred_element_type=F32)
        coefs = term if coefs is None else coefs + term
    same = iota((NVEC, size), 1) % count == iota((NVEC, size), 0) % count
    guesses = []
    for n, ref in enumerate(vectors):
        skip = ref.shape[0] - 2 * size
        wide_vectors = jnp.concatenate(
            [ref[skip : skip + size], ref[skip + size : skip + 2 * size]], axis=1
        )
        left = jnp.concatenate(
            [jnp.where(same, coefs[2 * n + q : 2 * n + q + 1, :size], 0.0) for q in range(2)],
            axis=0,
        )
        made = dot(left, wide_vectors)
        guesses.append(
            jnp.concatenate(
                [
                    made[:NVEC, :LANES] - made[NVEC:, LANES:],
                    made[:NVEC, LANES:] + made[NVEC:, :LANES],
                ],
                axis=0,
            )
        )
    own = guesses[0]
    near = [own]
    at = 1
    for c, axis in zip(counts, axes):
        near.extend(ahead_behind(guesses[at : at + c], axis))
        at += c
    aggregate = iota(own.shape, 1) % blocks
    near.append(
        jnp.where(
            aggregate == blocks - 1, pltpu.roll(own, blocks - 1, 1), pltpu.roll(own, LANES - 1, 1)
        )
    )
    near.append(
        jnp.where(aggregate == 0, pltpu.roll(own, LANES - blocks + 1, 1), pltpu.roll(own, 1, 1))
    )
    made_re, made_im = [], []
    for block in range(size // NVEC):
        acc_re = acc_im = None
        for d, value in enumerate(near):
            re, im = value[:NVEC], value[NVEC:]
            m_re, m_im = [read_block(p, d, block) for p in range(2)]
            got_re = m_re * re - m_im * im
            got_im = m_re * im + m_im * re
            acc_re = got_re if acc_re is None else acc_re + got_re
            acc_im = got_im if acc_im is None else acc_im + got_im
        row = iota((NVEC, LANES), 0) + block * NVEC
        at_home = (row % count) * per + iota((NVEC, LANES), 1) // blocks == row // count
        keep = 1.0 - middle_damping * middle_shift
        made_re.append(jnp.where(at_home, keep * own[:NVEC], 0.0) - middle_damping * acc_re)
        made_im.append(jnp.where(at_home, keep * own[NVEC:], 0.0) - middle_damping * acc_im)
    made = jnp.concatenate(
        [jnp.concatenate(made_re, axis=0), jnp.concatenate(made_im, axis=0)], axis=1
    )
    row_sum = one_hot(iota((NVEC, size), 1) // count == iota((NVEC, size), 0))
    summed = dot(row_sum, made)
    summed = jnp.concatenate([summed[:, :LANES], summed[:, LANES:]], axis=0)
    lane_sum = one_hot(
        iota((LANES, LANES), 0) % blocks == iota((LANES, LANES), 1) % blocks
    )
    update = dot(summed, lane_sum) + middle_damping * middle[...]
    lift = one_hot(iota((LANES, LANES), 0) == iota((LANES, LANES), 1) // BY, BF16)
    lifted = jnp.dot(update.astype(BF16), lift, preferred_element_type=F32)
    u_re, u_im = lifted[:NVEC], lifted[NVEC:]
    wide[...] = fine[...].astype(F32)
    sum_re, sum_im = [], []
    for i in range(HALF):
        re, im = strided_vectors(wide, i)
        sum_re.append(jnp.sum(re * u_re - im * u_im, axis=0, keepdims=True))
        sum_im.append(jnp.sum(re * u_im + im * u_re, axis=0, keepdims=True))
    out[...] = spinor[...] + jnp.concatenate(sum_re + sum_im, axis=0)


def third_kernel(counts, axes, blocks, shape, received, *refs):
    n_sites = 1 + sum(counts)
    held, spread, gather, matrix, refs = refs[:2], refs[2], refs[3], refs[4], refs[5:]
    vectors, refs = refs[:n_sites], refs[n_sites:]
    middle, fine, spinor, out, near, image, wide = refs
    nt, nz, nx = shape
    ta, gz = lax.axis_index("ta"), lax.axis_index("gz")
    total = received.shape[0]
    row, col = iota((2 * SUB, total), 0), iota((2 * SUB, total), 1)
    line = (ta ^ (row // 2 % nt)) * nz + (gz ^ (row // SUB))
    fold = one_hot((col // (2 * nx) == line) & (col % 2 == row % 2))
    r = dot(fold, received[...])
    apply = functools.partial(
        bottom_apply,
        near=near,
        image=image,
        spread=spread,
        gather=gather,
        held=held,
        width=nx * NVEC2,
    )
    f = apply(r)
    s = apply(f)
    rows = bottom_rows(nx, minimal_residual(r, f, s))
    size = NVEC * NVEC * blocks // LANES

    def read_block(p, d, block):
        return matrix[pl.ds((p * 9 + d) * size + block * NVEC, NVEC), :]

    middle_step(
        counts, axes, blocks, rows, vectors, middle, read_block, fine, spinor, out, wide
    )


def fourth_kernel(counts, axes, blocks, rows, *refs):
    n_sites = 1 + sum(counts)
    matrix, refs = refs[0], refs[1:]
    vectors, refs = refs[:n_sites], refs[n_sites:]
    middle, fine, spinor, out, wide = refs
    size = NVEC * NVEC * blocks // LANES

    def read_block(p, d, block):
        return matrix[pl.ds((p * 9 + d) * size + block * NVEC, NVEC), :]

    middle_step(
        counts, axes, blocks, rows[...], vectors, middle, read_block, fine, spinor, out, wide
    )


def vmem():
    return pl.BlockSpec(memory_space=pltpu.VMEM)


def top(rows):
    return pl.BlockSpec((rows, LANES), lambda i: (0, 0))


def shape_of(*dims):
    return jax.ShapeDtypeStruct(dims, F32)


def params(mib):
    return pltpu.CompilerParams(vmem_limit_bytes=mib * 2**20)


def line_solve(right, bottom_blocks):
    split = bottom_blocks.reshape((2, 7, -1, NVEC2, NVEC2))
    line = lax.all_gather(right, "xy", axis=1, tiled=False)

    def turned(v, axis, step):
        n = lax.axis_size(axis)
        return lax.ppermute(v, axis, [((i + step) % n, i) for i in range(n)])

    def product(blocks, v):
        return jnp.einsum("dxjk,dxk->xj", blocks, v, precision=HIGHEST)

    def apply(v):
        near = [v, turned(v, "ta", 1), turned(v, "ta", -1), turned(v, "gz", 1), turned(v, "gz", -1)]
        near = jnp.stack(near + [jnp.roll(v, -1, 1), jnp.roll(v, 1, 1)], axis=1)
        re = product(split[0], near[0]) - product(split[1], near[1])
        im = product(split[0], near[1]) + product(split[1], near[0])
        return bottom_shift * v + jnp.stack([re, im])

    first = apply(line)
    second = apply(first)

    def inner(u, w):
        return [jnp.sum(u[0] * w[0] + u[1] * w[1]), jnp.sum(u[0] * w[1] - u[1] * w[0])]

    sums = inner(first, first)[:1] + inner(second, second)[:1] + inner(first, second)
    sums = sums + inner(first, line) + inner(second, line)
    ff, ss, cr, ci, pr, pi, qr, qi = lax.psum(jnp.stack(sums), ("ta", "gz"))
    det = ff * ss - cr * cr - ci * ci
    a_re = (ss * pr - (cr * qr - ci * qi)) / det
    a_im = (ss * pi - (cr * qi + ci * qr)) / det
    b_re = (ff * qr - (cr * pr + ci * pi)) / det
    b_im = (ff * qi - (cr * pi - ci * pr)) / det

    def scaled(re, im, v):
        return jnp.stack([re * v[0] - im * v[1], re * v[1] + im * v[0]])

    solved = scaled(a_re, a_im, line) + scaled(b_re, b_im, first)
    return lax.dynamic_index_in_dim(solved, lax.axis_index("xy"), 1, keepdims=False)


def shards(source_field, gauge_links, fine_vectors, middle_blocks, middle_vectors, bottom_blocks):
    axes = ("ta", "gz", "xy")
    shape = tuple(lax.axis_size(a) for a in axes)
    nt, nz, nx = shape
    devices = nt * nz * nx
    blocks = source_field.shape[-1] // BY
    source = source_field.reshape(SPINOR, LANES)
    gauge = gauge_links.reshape(-1, LANES)
    fine = jnp.transpose(fine_vectors, (0, 1, 3, 4, 5, 6, 2, 7)).reshape(-1, LANES)
    matrix = middle_blocks.reshape(-1, LANES)
    vectors = middle_vectors.reshape(-1, LANES)
    size = vectors.shape[0]
    first, second, project, third = fine_tables()
    counts = [len(pairings(n)) for n in shape]
    gathered = nt == 4 and nz == 2 and 2 < nx and nx % 2 == 0 and nx * NVEC2 <= LANES

    halos = neighbours(source, axes)
    flat = [a for pair in halos for a in pair]
    tables = (first, second, project, third)
    loads = [jnp.asarray(a) for a in (source, gauge, vectors, fine) + tables]
    shapes = [jax.ShapeDtypeStruct(a.shape, a.dtype) for a in loads]
    scratch = []
    if gathered:
        loads.append(bottom_blocks.reshape(1, -1))
        shapes.append(shape_of(bottom_blocks.shape[-1] * 12 // LANES, LANES))
        scratch.append(pltpu.VMEM(loads[-1].shape, F32))
    loaded = pl.pallas_call(
        functools.partial(load_kernel, gathered),
        out_shape=tuple(shapes),
        in_specs=[pl.BlockSpec(memory_space=pltpu.HBM)] * len(loads),
        out_specs=(vmem(),) * len(loads),
        scratch_shapes=scratch + [pltpu.SemaphoreType.DMA((len(loads),))],
        compiler_params=params(4),
    )(*[pltpu.with_memory_space_constraint(a, pltpu.HBM) for a in loads])
    source, gauge, vectors, fine, first, second, project, third = loaded[:8]
    if gathered:
        line = loaded[8]
        beside = lax.ppermute(line, "ta", [(i, i ^ 1) for i in range(nt)])
        pair = jnp.concatenate([line, beside])
    payload = pl.pallas_call(
        functools.partial(first_kernel, counts, axes),
        out_shape=shape_of(SPINOR + size, LANES),
        in_specs=[vmem()] * (len(flat) + 5),
        out_specs=vmem(),
        compiler_params=params(8),
    )(source, *flat, gauge, vectors, first, second)

    near = neighbours(payload, axes)
    flat_near = [a for pair in near for a in pair]
    if gathered:
        other = lax.ppermute(pair, "ta", [(i, i ^ 2) for i in range(nt)])
        held = jnp.concatenate([pair, other])
        held = [held, lax.ppermute(held, "gz", [(i, i ^ 1) for i in range(nz)])]
    dests = devices if gathered else SUB
    residual, middle, sent = pl.pallas_call(
        functools.partial(second_kernel, counts, axes, blocks, gathered, dests),
        out_shape=(shape_of(SPINOR, LANES), shape_of(2 * NVEC, LANES), shape_of(2 * dests, LANES)),
        grid=(1,),
        in_specs=[vmem()] + [top(SPINOR)] * (1 + len(flat_near)) + [vmem()] * 5,
        out_specs=(vmem(), vmem(), vmem()),
        scratch_shapes=[pltpu.VMEM(fine.shape, F32)],
        compiler_params=params(8),
    )(source, payload, *flat_near, gauge, fine, vectors, project, third)

    if gathered:
        received = lax.all_to_all(sent.reshape(devices, 2, LANES), axes, 0, 0)
        received = received.reshape(2 * devices, LANES)
        lane = np.arange(nx * NVEC2 * NVEC2)
        k_lane = np.arange(LANES)[:, None]
        spread = k_lane == (lane // (NVEC2 * NVEC2) * NVEC2 + lane % NVEC2)[None]
        gather = k_lane == (lane // NVEC2)[None]
        spread, gather = jnp.asarray(spread, BF16), jnp.asarray(gather, BF16)
        solution = pl.pallas_call(
            functools.partial(third_kernel, counts, axes, blocks, shape),
            out_shape=shape_of(SPINOR, LANES),
            grid=(1,),
            in_specs=[vmem()] * (7 + len(flat_near)) + [vmem(), vmem(), top(SPINOR)],
            out_specs=vmem(),
            scratch_shapes=[
                pltpu.VMEM((6 * SUB, lane.size), F32),
                pltpu.VMEM((4 * SUB, lane.size), F32),
                pltpu.VMEM(fine.shape, F32),
            ],
            compiler_params=params(8),
        )(received, *held, spread, gather, matrix, vectors, *flat_near, middle, fine, payload)
    else:
        solved = line_solve(sent[:2, :NVEC2], bottom_blocks)
        solved = jnp.pad(solved, ((0, 0), (0, LANES - NVEC2)))
        rows = [solved] + [a for pair in neighbours(solved, axes) for a in pair]
        rows = jnp.concatenate(rows)
        rows = jnp.pad(rows, ((0, 2 * SUB - rows.shape[0]), (0, 0)))
        solution = pl.pallas_call(
            functools.partial(fourth_kernel, counts, axes, blocks),
            out_shape=shape_of(SPINOR, LANES),
            grid=(1,),
            in_specs=[vmem()] * (3 + len(flat_near)) + [vmem(), vmem(), top(SPINOR)],
            out_specs=vmem(),
            scratch_shapes=[pltpu.VMEM(fine.shape, F32)],
            compiler_params=params(16),
        )(rows, matrix, vectors, *flat_near, middle, fine, payload)
    return solution.reshape(source_field.shape), residual.reshape(source_field.shape)


def solution(mesh):
    return jax.shard_map(
        shards,
        mesh=mesh,
        in_specs=(
            P(None, None, None, "ta", "gz", "xy", None),
            P(None, None, None, None, "ta", "gz", "xy", None),
            P(None, None, None, None, "ta", "gz", "xy", None),
            P(None, None, None, "ta", "gz", "xy", None),
            P(None, None, "ta", "gz", "xy", None),
            P(None, None, "ta", "gz", None),
        ),
        out_specs=(
            P(None, None, None, "ta", "gz", "xy", None),
            P(None, None, None, "ta", "gz", "xy", None),
        ),
        check_vma=False,
    )
```

```python
import functools

import jax
import jax.numpy as jnp
import numpy as np
from jax import lax
from jax.experimental import pallas as pl
from jax.experimental.pallas import tpu as pltpu
from jax.sharding import PartitionSpec as P


BY = 4
NVEC = 24
NVEC2 = 24
SPINOR = 24
HALF = 12
LANES = 128
SUB = 8

quark_mass = 0.1
twist_mass = 0.1
fine_damping = 0.8
middle_damping = 0.4
middle_shift = 2.0
bottom_shift = 2.0
gamma = np.array(
    [
        [[0, 0, 1, 0], [0, 0, 0, 1], [1, 0, 0, 0], [0, 1, 0, 0]],
        [[0, 0, 1j, 0], [0, 0, 0, -1j], [-1j, 0, 0, 0], [0, 1j, 0, 0]],
        [[0, 0, 0, 1j], [0, 0, 1j, 0], [0, -1j, 0, 0], [-1j, 0, 0, 0]],
        [[0, 0, 0, -1], [0, 0, 1, 0], [0, 1, 0, 0], [-1, 0, 0, 0]],
    ],
    np.complex64,
)
HIGHEST = lax.Precision.HIGHEST
F32 = jnp.float32
BF16 = jnp.bfloat16


def real_form(matrix):
    return np.block([[matrix.real, -matrix.imag], [matrix.imag, matrix.real]])


def fine_tables():
    color = np.eye(3)
    project = np.zeros((2, 2, 3, 8, 8, SPINOR))
    rebuild = np.zeros((SPINOR, 2, 2, 3, 8))
    for m in range(4):
        for back in range(2):
            sign = -1.0 if back else 1.0
            way = 2 * m + back
            upper = np.eye(4)[:2] - sign * gamma[m][:2]
            project[:, :, :, way, way] = real_form(np.kron(upper, color)).reshape(2, 2, 3, SPINOR)
            lower = np.concatenate([np.eye(2), -sign * gamma[m][2:, :2]])
            rebuild[..., way] = real_form(np.kron(lower, color)).reshape(SPINOR, 2, 2, 3)
    project = project.reshape(HALF * 8, 8 * SPINOR)
    rebuild = rebuild.reshape(SPINOR, HALF * 8)
    return [jnp.asarray(t, BF16) for t in (project, rebuild)]


def twisted(x, straight, crossed):
    count = x.shape[0] // SPINOR
    pieces = []
    for i in range(count):
        pieces += [x[i * SPINOR + HALF : (i + 1) * SPINOR], x[i * SPINOR : i * SPINOR + HALF]]
    other = jnp.concatenate(pieces, axis=0)
    row = iota(x.shape, 0) % SPINOR
    sign = jnp.where((row % HALF < HALF // 2) != (row < HALF), crossed, -crossed)
    return straight * x + sign * other


def inverse_of(x, scale):
    mass = 4.0 + quark_mass
    norm = mass * mass + twist_mass * twist_mass
    return twisted(x, scale * mass / norm, -scale * twist_mass / norm)


def pairings(n):
    if n % 2:
        return [[((i + 1) % n, i) for i in range(n)], [(i, (i + 1) % n) for i in range(n)]]
    near = [(i, i ^ 1) for i in range(n)]
    far = [(i, (i + 1) % n if i % 2 else (i - 1) % n) for i in range(n)]
    return [near] if n == 2 else [near, far]


def neighbours(array, axes):
    found = []
    for axis in axes:
        pairs = pairings(lax.axis_size(axis))
        found.append(
            [
                lax.ppermute(array(axis, i) if callable(array) else array, axis, p)
                for i, p in enumerate(pairs)
            ]
        )
    return found


def load_kernel(has_line, *refs):
    sems = refs[-1]
    count = sems.shape[0]
    ins, outs = refs[:count], list(refs[count : 2 * count])
    if has_line:
        out, outs[-1] = outs[-1], refs[-2]
    copies = [pltpu.make_async_copy(ins[i], outs[i], sems.at[i]) for i in range(count)]
    for copy in reversed(copies):
        copy.start()
    if has_line:
        copies[-1].wait()
        source = outs[-1]
        chunks = out.shape[0] // 12
        even = lax.axis_index("ta") % 2 == 0
        for p in range(2):
            way = [
                source[:, (p * 7 + d) * chunks * LANES : (p * 7 + d + 1) * chunks * LANES]
                for d in range(7)
            ]
            ahead, behind = way[1], way[2]
            ways = [way[0], jnp.where(even, ahead, behind), jnp.where(even, behind, ahead)]
            ways += [way[3] + way[4], way[5], way[6]]
            for d, value in enumerate(ways):
                for c in range(chunks):
                    row = (p * 6 + d) * chunks + c
                    out[row : row + 1] = value[:, c * LANES : (c + 1) * LANES]
        copies = copies[:-1]
    for copy in copies:
        copy.wait()


def side_step(axis, which):
    n = lax.axis_size(axis)
    ahead = 1 if which == 0 else -1
    if n % 2:
        return ahead
    return ahead * (1 - 2 * (lax.axis_index(axis) % 2))


def ahead_behind(pair, axis):
    if len(pair) == 1:
        return pair[0], pair[0]
    n = lax.axis_size(axis)
    if n % 2:
        return pair[0], pair[1]
    even = lax.axis_index(axis) % 2 == 0
    return jnp.where(even, pair[0], pair[1]), jnp.where(even, pair[1], pair[0])


def parts(x, count):
    found = []
    for _ in range(count):
        found.append(x.astype(BF16))
        x = x - found[-1].astype(F32)
    return found


def table_left(table, x, count=2):
    n = x.shape[1]
    out = jnp.dot(table, jnp.concatenate(parts(x, count), axis=1), preferred_element_type=F32)
    return sum(out[:, i * n : (i + 1) * n] for i in range(count))


def table_right(x, table, count=2):
    m = x.shape[0]
    out = jnp.dot(jnp.concatenate(parts(x, count), axis=0), table, preferred_element_type=F32)
    return sum(out[i * m : (i + 1) * m] for i in range(count))


def product(a, b):
    m = a.shape[0]
    a_high, a_low = parts(a, 2)
    b_high, b_low = parts(b, 2)
    out = jnp.dot(jnp.concatenate([a_high, a_low], axis=0), b_high, preferred_element_type=F32)
    return out[:m] + out[m:] + jnp.dot(a_high, b_low, preferred_element_type=F32)


def iota(shape, dim):
    return lax.broadcasted_iota(jnp.int32, shape, dim)


def one_hot(condition, dtype=BF16):
    return jnp.where(condition, 1.0, 0.0).astype(dtype)


def hopping(spinor, halos, gauge, project, rebuild, axes, change=None):
    seen = []
    for pair, axis in zip(halos, axes):
        seen.extend(ahead_behind(pair, axis))
    seen.append(pltpu.roll(spinor, LANES - 1, 1))
    seen.append(pltpu.roll(spinor, 1, 1))
    seen = jnp.concatenate(seen, axis=0)
    half = table_left(project, seen if change is None else change(seen))
    rows = [[[None] * 3 for _ in range(2)] for _ in range(2)]
    for a in range(3):
        for b in range(3):
            link = [gauge[pl.ds(p * 72 + a * 3 + b, 8, stride=9), :] for p in range(2)]
            for s in range(2):
                re = half[(s * 3 + b) * 8 : (s * 3 + b) * 8 + 8]
                im = half[(6 + s * 3 + b) * 8 : (6 + s * 3 + b) * 8 + 8]
                out_re = link[0] * re - link[1] * im
                out_im = link[0] * im + link[1] * re
                for p, value in ((0, out_re), (1, out_im)):
                    old = rows[p][s][a]
                    rows[p][s][a] = value if old is None else old + value
    rows = [rows[p][s][a] for p in range(2) for s in range(2) for a in range(3)]
    return table_left(rebuild, jnp.concatenate(rows, axis=0))


def first_kernel(counts, axes, *refs):
    source, refs = refs[0], refs[1:]
    halos, at = [], 0
    for count in counts:
        halos.append([r[...] for r in refs[at : at + count]])
        at += count
    gauge, vectors, project, rebuild, alone, out = refs[at:]
    value = source[...]
    start = functools.partial(inverse_of, scale=fine_damping)
    hop = hopping(value, halos, gauge, project[...], rebuild[...], axes, start)
    result = inverse_of(
        fine_damping * (2.0 - fine_damping) * value + 0.5 * fine_damping * hop, 1.0
    )
    alone[...] = result
    out[:SPINOR] = result
    size = out.shape[0] - SPINOR
    out[SPINOR:] = vectors[pl.ds(vectors.shape[0] - size, size), :]


def strided_vectors(fine, i):
    row = (i % 3) * 4 + i // 3
    return [fine[pl.ds(p * NVEC * HALF + row, NVEC, stride=HALF), :] for p in range(2)]


def second_kernel(counts, axes, blocks, place, dests, *refs):
    source, own, refs = refs[0], refs[1], refs[2:]
    halos, at = [], 0
    for count in counts:
        halos.append([r[...] for r in refs[at : at + count]])
        at += count
    gauge, fine, vectors, project, rebuild, out, middle, sent, wide = refs[at:]
    spinor = own[...]
    hop = hopping(spinor, halos, gauge, project[...], rebuild[...], axes)
    residual = source[...] - twisted(spinor, 4.0 + quark_mass, twist_mass) + 0.5 * hop
    out[...] = residual
    low = residual.astype(BF16).astype(F32)
    wide[...] = fine[...].astype(F32)
    sum_re = jnp.zeros((NVEC, LANES), F32)
    sum_im = jnp.zeros((NVEC, LANES), F32)
    for i in range(HALF):
        re, im = strided_vectors(wide, i)
        low_re, low_im = low[i : i + 1], low[HALF + i : HALF + i + 1]
        sum_re = sum_re + re * low_re + im * low_im
        sum_im = sum_im + re * low_im - im * low_re
    group = iota((LANES, LANES), 1) % blocks == iota((LANES, LANES), 0) // BY
    right = table_right(jnp.concatenate([sum_re, sum_im], axis=0), one_hot(group))
    middle[...] = right
    per = LANES // blocks
    count = NVEC // per
    keep = iota((NVEC, LANES), 1) // blocks == iota((NVEC, LANES), 0) % per
    pick = one_hot(iota((NVEC, NVEC), 1) // per == iota((NVEC, NVEC), 0) % count)
    kept = [jnp.where(keep, right[p * NVEC : (p + 1) * NVEC], 0.0) for p in range(2)]
    pattern = table_left(pick, jnp.concatenate(kept, axis=1))
    pat_re, pat_im = pattern[:, :LANES], pattern[:, LANES:]
    size = NVEC2 * count
    skip = vectors.shape[0] - 2 * size
    made_re, made_im = [], []
    for block in range(size // NVEC):
        re = vectors[pl.ds(skip + block * NVEC, NVEC), :]
        im = vectors[pl.ds(skip + size + block * NVEC, NVEC), :]
        made_re.append(re * pat_re + im * pat_im)
        made_im.append(re * pat_im - im * pat_re)
    made = jnp.concatenate(made_re + made_im, axis=0)
    summed = table_right(made, jnp.ones((LANES, LANES), BF16))
    shift = lax.axis_index("xy") * NVEC2 if place else 0
    home = iota((size, LANES), 1) == iota((size, LANES), 0) // count + shift
    line = [
        jnp.sum(jnp.where(home, summed[p * size : (p + 1) * size], 0.0), axis=0, keepdims=True)
        for p in range(2)
    ]
    both = jnp.where(iota((SUB, LANES), 0) % 2 == 0, line[0], line[1])
    for i in range(2 * dests // SUB):
        sent[i * SUB : (i + 1) * SUB] = both


def exchanged(x, step):
    rows = x.shape[0]
    if rows == 2 * step:
        return pltpu.roll(x, step, 0)
    up, down = pltpu.roll(x, rows - step, 0), pltpu.roll(x, step, 0)
    return jnp.where(iota(x.shape, 0) // step % 2 == 0, up, down)


def bottom_apply(v, near, image, spread, gather, held, width):
    lane = iota(v.shape, 1)
    edge = width - NVEC2
    up = jnp.where(lane < edge, pltpu.roll(v, LANES - NVEC2, 1), pltpu.roll(v, edge, 1))
    down = jnp.where(lane >= NVEC2, pltpu.roll(v, NVEC2, 1), pltpu.roll(v, LANES - edge, 1))
    rows = jnp.concatenate([v, jnp.where(lane < width, up, 0.0), down], axis=0)
    near[...] = table_right(rows, spread[...], 3)
    chunks = near.shape[1] // LANES
    stride = 6 * chunks
    for c in range(chunks):
        here = pl.ds(c * LANES, LANES)
        seen = [near[i * SUB : (i + 1) * SUB, here] for i in range(6)]
        turned = [exchanged(x, 1) for x in seen]
        for core in range(2):
            acc = [None, None]
            for n, rows in enumerate((seen, turned)):
                beside = exchanged(rows[core], 2)
                ways = [rows[core], beside, pltpu.roll(beside, 4, 0), rows[1 - core]]
                ways += [rows[2 + core], rows[4 + core]]
                for d, value in enumerate(ways):
                    block = held[core][pl.ds(d * chunks + c, SUB, stride=stride), :]
                    got = block * value
                    acc[n] = got if acc[n] is None else acc[n] + got
                image[(2 * n + core) * SUB : (2 * n + core + 1) * SUB, here] = acc[n]
    total = table_right(image[...], gather[...], 3)
    first, second = total[: 2 * SUB], total[2 * SUB :]
    re = first - exchanged(first, 1)
    im = second + exchanged(second, 1)
    return bottom_shift * v + jnp.where(iota(v.shape, 0) % 2 == 0, re, im)


def whole_sum(x):
    return jnp.sum(jnp.sum(x, axis=1, keepdims=True), axis=0, keepdims=True)


def minimal_residual(r, f, s):
    sign = jnp.where(iota(r.shape, 0) % 2 == 0, 1.0, -1.0)
    r_turn, s_turn, f_turn = exchanged(r, 1), exchanged(s, 1), exchanged(f, 1)
    ff = whole_sum(f * f)
    ss = whole_sum(s * s)
    cross_re = whole_sum(f * s)
    cross_im = whole_sum(sign * f * s_turn)
    one_re = whole_sum(f * r)
    one_im = whole_sum(sign * f * r_turn)
    two_re = whole_sum(s * r)
    two_im = whole_sum(sign * s * r_turn)
    determinant = ff * ss - cross_re * cross_re - cross_im * cross_im
    a_re = (ss * one_re - (cross_re * two_re - cross_im * two_im)) / determinant
    a_im = (ss * one_im - (cross_re * two_im + cross_im * two_re)) / determinant
    b_re = (ff * two_re - (cross_re * one_re + cross_im * one_im)) / determinant
    b_im = (ff * two_im - (cross_re * one_im - cross_im * one_re)) / determinant
    return a_re * r + b_re * f - sign * (a_im * r_turn + b_im * f_turn)


def bottom_rows(nx, solution):
    rows = jnp.concatenate(
        [
            solution[0:4],
            solution[6:10],
            solution[0:2],
            solution[0:2],
            jnp.zeros((4, LANES), F32),
        ],
        axis=0,
    )
    x = lax.axis_index("xy")

    def turned(step):
        place = lax.rem(x + step + nx, nx)
        return pltpu.roll(rows, lax.rem(LANES - NVEC2 * place, LANES), 1)

    site = iota(rows.shape, 0) // 2
    near, far = turned(side_step("xy", 0)), turned(side_step("xy", 1))
    result = jnp.where(site == 4, near, jnp.where(site == 5, far, turned(0)))
    return jnp.where(iota(result.shape, 1) < NVEC2, result, 0.0)


def middle_step(counts, axes, blocks, rows, vectors, middle, read_block, fine, spinor, out, wide):
    per = LANES // blocks
    count = NVEC // per
    size = NVEC2 * count
    spread = one_hot(
        (iota((LANES, 2 * LANES), 0) == iota((LANES, 2 * LANES), 1) // count)
        & (iota((LANES, 2 * LANES), 1) < size)
    )
    coefs = table_right(rows, spread, 3)
    same = iota((NVEC, size), 1) % count == iota((NVEC, size), 0) % count
    guesses = []
    for n, ref in enumerate(vectors):
        skip = ref.shape[0] - 2 * size
        wide_vectors = jnp.concatenate(
            [ref[skip : skip + size], ref[skip + size : skip + 2 * size]], axis=1
        )
        left = jnp.concatenate(
            [jnp.where(same, coefs[2 * n + q : 2 * n + q + 1, :size], 0.0) for q in range(2)],
            axis=0,
        )
        made = product(left, wide_vectors)
        guesses.append(
            jnp.concatenate(
                [
                    made[:NVEC, :LANES] - made[NVEC:, LANES:],
                    made[:NVEC, LANES:] + made[NVEC:, :LANES],
                ],
                axis=0,
            )
        )
    own = guesses[0]
    near = [own]
    at = 1
    for c, axis in zip(counts, axes):
        near.extend(ahead_behind(guesses[at : at + c], axis))
        at += c
    aggregate = iota(own.shape, 1) % blocks
    near.append(
        jnp.where(
            aggregate == blocks - 1, pltpu.roll(own, blocks - 1, 1), pltpu.roll(own, LANES - 1, 1)
        )
    )
    near.append(
        jnp.where(aggregate == 0, pltpu.roll(own, LANES - blocks + 1, 1), pltpu.roll(own, 1, 1))
    )
    count_blocks = size // NVEC
    sums = [[None, None] for _ in range(count_blocks)]
    for d, value in enumerate(near):
        re, im = value[:NVEC], value[NVEC:]
        for block in range(count_blocks):
            m_re, m_im = [read_block(p, d, block) for p in range(2)]
            got = [m_re * re - m_im * im, m_re * im + m_im * re]
            sums[block] = [g if a is None else a + g for a, g in zip(sums[block], got)]
    made_re, made_im = [], []
    for block in range(count_blocks):
        acc_re, acc_im = sums[block]
        row = iota((NVEC, LANES), 0) + block * NVEC
        at_home = (row % count) * per + iota((NVEC, LANES), 1) // blocks == row // count
        keep = 1.0 - middle_damping * middle_shift
        made_re.append(jnp.where(at_home, keep * own[:NVEC], 0.0) - middle_damping * acc_re)
        made_im.append(jnp.where(at_home, keep * own[NVEC:], 0.0) - middle_damping * acc_im)
    made = jnp.concatenate(
        [jnp.concatenate(made_re, axis=0), jnp.concatenate(made_im, axis=0)], axis=1
    )
    row_sum = one_hot(iota((NVEC, size), 1) // count == iota((NVEC, size), 0))
    summed = table_left(row_sum, made)
    summed = jnp.concatenate([summed[:, :LANES], summed[:, LANES:]], axis=0)
    lane_sum = one_hot(
        iota((LANES, LANES), 0) % blocks == iota((LANES, LANES), 1) % blocks
    )
    update = table_right(summed, lane_sum) + middle_damping * middle[...]
    lift = one_hot(iota((LANES, LANES), 0) == iota((LANES, LANES), 1) // BY)
    lifted = jnp.dot(update.astype(BF16), lift, preferred_element_type=F32)
    u_re, u_im = lifted[:NVEC], lifted[NVEC:]
    wide[...] = fine[...].astype(F32)
    sum_re, sum_im = [], []
    for i in range(HALF):
        re, im = strided_vectors(wide, i)
        sum_re.append(jnp.sum(re * u_re - im * u_im, axis=0, keepdims=True))
        sum_im.append(jnp.sum(re * u_im + im * u_re, axis=0, keepdims=True))
    out[...] = spinor[...] + jnp.concatenate(sum_re + sum_im, axis=0)


def third_kernel(counts, axes, blocks, shape, received, *refs):
    n_sites = 1 + sum(counts)
    held, spread, gather, matrix, refs = refs[:2], refs[2], refs[3], refs[4], refs[5:]
    vectors, refs = refs[:n_sites], refs[n_sites:]
    middle, fine, spinor, out, near, image, wide = refs
    nt, nz, nx = shape
    ta, gz = lax.axis_index("ta"), lax.axis_index("gz")
    total = received.shape[0]
    row, col = iota((2 * SUB, total), 0), iota((2 * SUB, total), 1)
    line = (ta ^ (row // 2 % nt)) * nz + (gz ^ (row // SUB))
    fold = one_hot((col // (2 * nx) == line) & (col % 2 == row % 2))
    r = table_left(fold, received[...], 3)
    apply = functools.partial(
        bottom_apply,
        near=near,
        image=image,
        spread=spread,
        gather=gather,
        held=held,
        width=nx * NVEC2,
    )
    f = apply(r)
    s = apply(f)
    rows = bottom_rows(nx, minimal_residual(r, f, s))
    size = NVEC * NVEC * blocks // LANES

    def read_block(p, d, block):
        return matrix[pl.ds((p * 9 + d) * size + block * NVEC, NVEC), :]

    middle_step(
        counts, axes, blocks, rows, vectors, middle, read_block, fine, spinor, out, wide
    )


def fourth_kernel(counts, axes, blocks, rows, *refs):
    n_sites = 1 + sum(counts)
    matrix, refs = refs[0], refs[1:]
    vectors, refs = refs[:n_sites], refs[n_sites:]
    middle, fine, spinor, out, wide = refs
    size = NVEC * NVEC * blocks // LANES

    def read_block(p, d, block):
        return matrix[pl.ds((p * 9 + d) * size + block * NVEC, NVEC), :]

    middle_step(
        counts, axes, blocks, rows[...], vectors, middle, read_block, fine, spinor, out, wide
    )


def vmem():
    return pl.BlockSpec(memory_space=pltpu.VMEM)


def top(rows):
    return pl.BlockSpec((rows, LANES), lambda i: (0, 0))


def shape_of(*dims):
    return jax.ShapeDtypeStruct(dims, F32)


def params(mib):
    return pltpu.CompilerParams(vmem_limit_bytes=mib * 2**20)


def line_solve(right, bottom_blocks):
    split = bottom_blocks.reshape((2, 7, -1, NVEC2, NVEC2))
    line = lax.all_gather(right, "xy", axis=1, tiled=False)

    def turned(v, axis, step):
        n = lax.axis_size(axis)
        return lax.ppermute(v, axis, [((i + step) % n, i) for i in range(n)])

    def product(blocks, v):
        return jnp.einsum("dxjk,dxk->xj", blocks, v, precision=HIGHEST)

    def apply(v):
        near = [v, turned(v, "ta", 1), turned(v, "ta", -1), turned(v, "gz", 1), turned(v, "gz", -1)]
        near = jnp.stack(near + [jnp.roll(v, -1, 1), jnp.roll(v, 1, 1)], axis=1)
        re = product(split[0], near[0]) - product(split[1], near[1])
        im = product(split[0], near[1]) + product(split[1], near[0])
        return bottom_shift * v + jnp.stack([re, im])

    first = apply(line)
    second = apply(first)

    def inner(u, w):
        return [jnp.sum(u[0] * w[0] + u[1] * w[1]), jnp.sum(u[0] * w[1] - u[1] * w[0])]

    sums = inner(first, first)[:1] + inner(second, second)[:1] + inner(first, second)
    sums = sums + inner(first, line) + inner(second, line)
    ff, ss, cr, ci, pr, pi, qr, qi = lax.psum(jnp.stack(sums), ("ta", "gz"))
    det = ff * ss - cr * cr - ci * ci
    a_re = (ss * pr - (cr * qr - ci * qi)) / det
    a_im = (ss * pi - (cr * qi + ci * qr)) / det
    b_re = (ff * qr - (cr * pr + ci * pi)) / det
    b_im = (ff * qi - (cr * pi - ci * pr)) / det

    def scaled(re, im, v):
        return jnp.stack([re * v[0] - im * v[1], re * v[1] + im * v[0]])

    solved = scaled(a_re, a_im, line) + scaled(b_re, b_im, first)
    return lax.dynamic_index_in_dim(solved, lax.axis_index("xy"), 1, keepdims=False)


def shards(source_field, gauge_links, fine_vectors, middle_blocks, middle_vectors, bottom_blocks):
    axes = ("ta", "gz", "xy")
    shape = tuple(lax.axis_size(a) for a in axes)
    nt, nz, nx = shape
    devices = nt * nz * nx
    blocks = source_field.shape[-1] // BY
    source = source_field.reshape(SPINOR, LANES)
    gauge = gauge_links.reshape(-1, LANES)
    fine = jnp.transpose(fine_vectors, (0, 1, 3, 4, 5, 6, 2, 7)).reshape(-1, LANES)
    matrix = middle_blocks.reshape(-1, LANES)
    vectors = middle_vectors.reshape(-1, LANES)
    size = vectors.shape[0]
    project, rebuild = fine_tables()
    counts = [len(pairings(n)) for n in shape]
    gathered = nt == 4 and nz == 2 and 2 < nx and nx % 2 == 0 and nx * NVEC2 <= LANES

    halos = neighbours(source, axes)
    flat = [a for pair in halos for a in pair]
    loads = [source, gauge, fine, project, rebuild, vectors]
    shapes = [jax.ShapeDtypeStruct(a.shape, a.dtype) for a in loads]
    scratch = []
    depth = 0
    if gathered:
        depth = bottom_blocks.shape[-1] * 12 // LANES
        loads.append(bottom_blocks.reshape(1, -1))
        shapes.append(shape_of(depth, LANES))
        scratch.append(pltpu.VMEM(loads[-1].shape, F32))
    loaded = pl.pallas_call(
        functools.partial(load_kernel, gathered),
        out_shape=tuple(shapes),
        in_specs=[pl.BlockSpec(memory_space=pltpu.HBM)] * len(loads),
        out_specs=(vmem(),) * len(shapes),
        scratch_shapes=scratch + [pltpu.SemaphoreType.DMA((len(loads),))],
        compiler_params=params(4),
    )(*[pltpu.with_memory_space_constraint(a, pltpu.HBM) for a in loads])
    source, gauge, fine, project, rebuild, mine = loaded[:6]
    if gathered:
        line = loaded[6]
        beside = lax.ppermute(line, "ta", [(i, i ^ 1) for i in range(nt)])
        pair = jnp.concatenate([line, beside])
    spinor, payload = pl.pallas_call(
        functools.partial(first_kernel, counts, axes),
        out_shape=(shape_of(SPINOR, LANES), shape_of(SPINOR + size, LANES)),
        in_specs=[vmem()] * (len(flat) + 5),
        out_specs=(vmem(), vmem()),
        compiler_params=params(8),
    )(source, *flat, gauge, mine, project, rebuild)

    alone = (("ta", 0), ("xy", 1)) if gathered else ()
    near = neighbours(lambda axis, i: spinor if (axis, i) in alone else payload, axes)
    flat_near = [a for pair in near for a in pair]
    near_vectors = list(flat_near)
    if gathered:
        other = lax.ppermute(pair, "ta", [(i, i ^ 2) for i in range(nt)])
        near_vectors[0] = lax.ppermute(vectors, "ta", pairings(nt)[0])
        near_vectors[-1] = lax.ppermute(vectors, "xy", pairings(nx)[1])
    dests = devices if gathered else SUB
    residual, middle, sent = pl.pallas_call(
        functools.partial(second_kernel, counts, axes, blocks, gathered, dests),
        out_shape=(shape_of(SPINOR, LANES), shape_of(2 * NVEC, LANES), shape_of(2 * dests, LANES)),
        grid=(1,),
        in_specs=[vmem()] + [top(SPINOR)] * (1 + len(flat_near)) + [vmem()] * 5,
        out_specs=(vmem(), vmem(), vmem()),
        scratch_shapes=[pltpu.VMEM(fine.shape, F32)],
        compiler_params=params(8),
    )(source, spinor, *flat_near, gauge, fine, mine, project, rebuild)

    if gathered:
        received = lax.all_to_all(sent.reshape(devices, 2, LANES), axes, 0, 0)
        received = received.reshape(2 * devices, LANES)
        received, pair, other = lax.optimization_barrier((received, pair, other))
        held = jnp.concatenate([pair, other])
        held = [held, lax.ppermute(held, "gz", pairings(nz)[0])]
        lane = np.arange(nx * NVEC2 * NVEC2)
        k_lane = np.arange(LANES)[:, None]
        spread = k_lane == (lane // (NVEC2 * NVEC2) * NVEC2 + lane % NVEC2)[None]
        gather = k_lane.T == (lane // NVEC2)[:, None]
        spread, gather = jnp.asarray(spread, BF16), jnp.asarray(gather, BF16)
        solution = pl.pallas_call(
            functools.partial(third_kernel, counts, axes, blocks, shape),
            out_shape=shape_of(SPINOR, LANES),
            grid=(1,),
            in_specs=[vmem()] * (7 + len(flat_near)) + [vmem(), vmem(), top(SPINOR)],
            out_specs=vmem(),
            scratch_shapes=[
                pltpu.VMEM((6 * SUB, lane.size), F32),
                pltpu.VMEM((4 * SUB, lane.size), F32),
                pltpu.VMEM(fine.shape, F32),
            ],
            compiler_params=params(8),
        )(received, *held, spread, gather, matrix, mine, *near_vectors, middle, fine, spinor)
    else:
        solved = line_solve(sent[:2, :NVEC2], bottom_blocks)
        solved = jnp.pad(solved, ((0, 0), (0, LANES - NVEC2)))
        rows = [solved] + [a for pair in neighbours(solved, axes) for a in pair]
        rows = jnp.concatenate(rows)
        rows = jnp.pad(rows, ((0, 2 * SUB - rows.shape[0]), (0, 0)))
        solution = pl.pallas_call(
            functools.partial(fourth_kernel, counts, axes, blocks),
            out_shape=shape_of(SPINOR, LANES),
            grid=(1,),
            in_specs=[vmem()] * (3 + len(flat_near)) + [vmem(), vmem(), top(SPINOR)],
            out_specs=vmem(),
            scratch_shapes=[pltpu.VMEM(fine.shape, F32)],
            compiler_params=params(16),
        )(rows, matrix, mine, *near_vectors, middle, fine, spinor)
    return solution.reshape(source_field.shape), residual.reshape(source_field.shape)


def solution(mesh):
    return jax.shard_map(
        shards,
        mesh=mesh,
        in_specs=(
            P(None, None, None, "ta", "gz", "xy", None),
            P(None, None, None, None, "ta", "gz", "xy", None),
            P(None, None, None, None, "ta", "gz", "xy", None),
            P(None, None, None, "ta", "gz", "xy", None),
            P(None, None, "ta", "gz", "xy", None),
            P(None, None, "ta", "gz", None),
        ),
        out_specs=(
            P(None, None, None, "ta", "gz", "xy", None),
            P(None, None, None, "ta", "gz", "xy", None),
        ),
        check_vma=False,
    )
```

```python
import functools

import jax
import jax.numpy as jnp
import numpy as np
from jax import lax
from jax.experimental import pallas as pl
from jax.experimental.pallas import tpu as pltpu
from jax.sharding import PartitionSpec as P


BY = 4
NVEC = 24
NVEC2 = 24
SPINOR = 24
HALF = 12
LANES = 128
SUB = 8

quark_mass = 0.1
twist_mass = 0.1
fine_damping = 0.8
middle_damping = 0.4
middle_shift = 2.0
bottom_shift = 2.0
gamma = np.array(
    [
        [[0, 0, 1, 0], [0, 0, 0, 1], [1, 0, 0, 0], [0, 1, 0, 0]],
        [[0, 0, 1j, 0], [0, 0, 0, -1j], [-1j, 0, 0, 0], [0, 1j, 0, 0]],
        [[0, 0, 0, 1j], [0, 0, 1j, 0], [0, -1j, 0, 0], [-1j, 0, 0, 0]],
        [[0, 0, 0, -1], [0, 0, 1, 0], [0, 1, 0, 0], [-1, 0, 0, 0]],
    ],
    np.complex64,
)
HIGHEST = lax.Precision.HIGHEST
F32 = jnp.float32
BF16 = jnp.bfloat16


def real_form(matrix):
    return np.block([[matrix.real, -matrix.imag], [matrix.imag, matrix.real]])


def fine_tables():
    color = np.eye(3)
    project = np.zeros((2, 2, 3, 8, 8, SPINOR))
    rebuild = np.zeros((SPINOR, 2, 2, 3, 8))
    for m in range(4):
        for back in range(2):
            sign = -1.0 if back else 1.0
            way = 2 * m + back
            upper = np.eye(4)[:2] - sign * gamma[m][:2]
            project[:, :, :, way, way] = real_form(np.kron(upper, color)).reshape(2, 2, 3, SPINOR)
            lower = np.concatenate([np.eye(2), -sign * gamma[m][2:, :2]])
            rebuild[..., way] = real_form(np.kron(lower, color)).reshape(SPINOR, 2, 2, 3)
    project = project.reshape(HALF * 8, 8 * SPINOR)
    rebuild = rebuild.reshape(SPINOR, HALF * 8)
    return [jnp.asarray(t, BF16) for t in (project, rebuild)]


def twisted(x, straight, crossed):
    count = x.shape[0] // SPINOR
    pieces = []
    for i in range(count):
        pieces += [x[i * SPINOR + HALF : (i + 1) * SPINOR], x[i * SPINOR : i * SPINOR + HALF]]
    other = jnp.concatenate(pieces, axis=0)
    row = iota(x.shape, 0) % SPINOR
    sign = jnp.where((row % HALF < HALF // 2) != (row < HALF), crossed, -crossed)
    return straight * x + sign * other


def inverse_of(x, scale):
    mass = 4.0 + quark_mass
    norm = mass * mass + twist_mass * twist_mass
    return twisted(x, scale * mass / norm, -scale * twist_mass / norm)


def pairings(n):
    if n % 2:
        return [[((i + 1) % n, i) for i in range(n)], [(i, (i + 1) % n) for i in range(n)]]
    near = [(i, i ^ 1) for i in range(n)]
    far = [(i, (i + 1) % n if i % 2 else (i - 1) % n) for i in range(n)]
    return [near] if n == 2 else [near, far]


def neighbours(array, axes):
    found = []
    for axis in axes:
        pairs = pairings(lax.axis_size(axis))
        found.append(
            [
                lax.ppermute(array(axis, i) if callable(array) else array, axis, p)
                for i, p in enumerate(pairs)
            ]
        )
    return found


def load_kernel(has_line, *refs):
    sems = refs[-1]
    count = sems.shape[0]
    ins, outs = refs[:count], list(refs[count : 2 * count])
    if has_line:
        out, outs[-1] = outs[-1], refs[-2]
    copies = [pltpu.make_async_copy(ins[i], outs[i], sems.at[i]) for i in range(count)]
    for copy in reversed(copies):
        copy.start()
    if has_line:
        copies[-1].wait()
        source = outs[-1]
        chunks = out.shape[0] // 12
        even = lax.axis_index("ta") % 2 == 0
        for p in range(2):
            way = [
                source[:, (p * 7 + d) * chunks * LANES : (p * 7 + d + 1) * chunks * LANES]
                for d in range(7)
            ]
            ahead, behind = way[1], way[2]
            ways = [way[0], jnp.where(even, ahead, behind), jnp.where(even, behind, ahead)]
            ways += [way[3] + way[4], way[5], way[6]]
            for d, value in enumerate(ways):
                for c in range(chunks):
                    row = (p * 6 + d) * chunks + c
                    out[row : row + 1] = value[:, c * LANES : (c + 1) * LANES]
        copies = copies[:-1]
    for copy in copies:
        copy.wait()


def side_step(axis, which):
    n = lax.axis_size(axis)
    ahead = 1 if which == 0 else -1
    if n % 2:
        return ahead
    return ahead * (1 - 2 * (lax.axis_index(axis) % 2))


def ahead_behind(pair, axis):
    if len(pair) == 1:
        return pair[0], pair[0]
    n = lax.axis_size(axis)
    if n % 2:
        return pair[0], pair[1]
    even = lax.axis_index(axis) % 2 == 0
    return jnp.where(even, pair[0], pair[1]), jnp.where(even, pair[1], pair[0])


def parts(x, count):
    found = []
    for _ in range(count):
        found.append(x.astype(BF16))
        x = x - found[-1].astype(F32)
    return found


def table_left(table, x, count=2):
    n = x.shape[1]
    out = jnp.dot(table, jnp.concatenate(parts(x, count), axis=1), preferred_element_type=F32)
    return sum(out[:, i * n : (i + 1) * n] for i in range(count))


def table_right(x, table, count=2):
    m = x.shape[0]
    out = jnp.dot(jnp.concatenate(parts(x, count), axis=0), table, preferred_element_type=F32)
    return sum(out[i * m : (i + 1) * m] for i in range(count))


def product(a, b):
    m = a.shape[0]
    a_high, a_low = parts(a, 2)
    b_high, b_low = parts(b, 2)
    out = jnp.dot(jnp.concatenate([a_high, a_low], axis=0), b_high, preferred_element_type=F32)
    return out[:m] + out[m:] + jnp.dot(a_high, b_low, preferred_element_type=F32)


def iota(shape, dim):
    return lax.broadcasted_iota(jnp.int32, shape, dim)


def one_hot(condition, dtype=BF16):
    return jnp.where(condition, 1.0, 0.0).astype(dtype)


def hopping(spinor, halos, gauge, project, rebuild, axes, change=None):
    seen = []
    for pair, axis in zip(halos, axes):
        seen.extend(ahead_behind(pair, axis))
    seen.append(pltpu.roll(spinor, LANES - 1, 1))
    seen.append(pltpu.roll(spinor, 1, 1))
    seen = jnp.concatenate(seen, axis=0)
    half = table_left(project, seen if change is None else change(seen))
    rows = [[[None] * 3 for _ in range(2)] for _ in range(2)]
    for a in range(3):
        for b in range(3):
            link = [gauge[pl.ds(p * 72 + a * 3 + b, 8, stride=9), :] for p in range(2)]
            for s in range(2):
                re = half[(s * 3 + b) * 8 : (s * 3 + b) * 8 + 8]
                im = half[(6 + s * 3 + b) * 8 : (6 + s * 3 + b) * 8 + 8]
                out_re = link[0] * re - link[1] * im
                out_im = link[0] * im + link[1] * re
                for p, value in ((0, out_re), (1, out_im)):
                    old = rows[p][s][a]
                    rows[p][s][a] = value if old is None else old + value
    rows = [rows[p][s][a] for p in range(2) for s in range(2) for a in range(3)]
    return table_left(rebuild, jnp.concatenate(rows, axis=0))


def first_kernel(counts, axes, *refs):
    source, refs = refs[0], refs[1:]
    halos, at = [], 0
    for count in counts:
        halos.append([r[:SPINOR] for r in refs[at : at + count]])
        at += count
    gauge, vectors, project, rebuild, alone, out = refs[at:]
    value = source[...]
    start = functools.partial(inverse_of, scale=fine_damping)
    hop = hopping(value, halos, gauge, project[...], rebuild[...], axes, start)
    result = inverse_of(
        fine_damping * (2.0 - fine_damping) * value + 0.5 * fine_damping * hop, 1.0
    )
    alone[...] = result
    out[:SPINOR] = result
    size = out.shape[0] - SPINOR
    out[SPINOR:] = vectors[pl.ds(vectors.shape[0] - size, size), :]


def strided_vectors(fine, i):
    row = (i % 3) * 4 + i // 3
    return [fine[pl.ds(p * NVEC * HALF + row, NVEC, stride=HALF), :] for p in range(2)]


def second_kernel(counts, axes, blocks, place, dests, *refs):
    source, own, refs = refs[0], refs[1], refs[2:]
    halos, at = [], 0
    for count in counts:
        halos.append([r[:SPINOR] for r in refs[at : at + count]])
        at += count
    gauge, fine, vectors, project, rebuild, out, middle, sent, wide = refs[at:]
    spinor = own[...]
    hop = hopping(spinor, halos, gauge, project[...], rebuild[...], axes)
    residual = source[...] - twisted(spinor, 4.0 + quark_mass, twist_mass) + 0.5 * hop
    out[...] = residual
    low = residual.astype(BF16).astype(F32)
    wide[...] = fine[...].astype(F32)
    sum_re = jnp.zeros((NVEC, LANES), F32)
    sum_im = jnp.zeros((NVEC, LANES), F32)
    for i in range(HALF):
        re, im = strided_vectors(wide, i)
        low_re, low_im = low[i : i + 1], low[HALF + i : HALF + i + 1]
        sum_re = sum_re + re * low_re + im * low_im
        sum_im = sum_im + re * low_im - im * low_re
    group = iota((LANES, LANES), 1) % blocks == iota((LANES, LANES), 0) // BY
    right = table_right(jnp.concatenate([sum_re, sum_im], axis=0), one_hot(group))
    middle[...] = right
    per = LANES // blocks
    count = NVEC // per
    keep = iota((NVEC, LANES), 1) // blocks == iota((NVEC, LANES), 0) % per
    pick = one_hot(iota((NVEC, NVEC), 1) // per == iota((NVEC, NVEC), 0) % count)
    kept = [jnp.where(keep, right[p * NVEC : (p + 1) * NVEC], 0.0) for p in range(2)]
    pattern = table_left(pick, jnp.concatenate(kept, axis=1))
    pat_re, pat_im = pattern[:, :LANES], pattern[:, LANES:]
    size = NVEC2 * count
    skip = vectors.shape[0] - 2 * size
    made_re, made_im = [], []
    for block in range(size // NVEC):
        re = vectors[pl.ds(skip + block * NVEC, NVEC), :]
        im = vectors[pl.ds(skip + size + block * NVEC, NVEC), :]
        made_re.append(re * pat_re + im * pat_im)
        made_im.append(re * pat_im - im * pat_re)
    made = jnp.concatenate(made_re + made_im, axis=0)
    summed = table_right(made, jnp.ones((LANES, LANES), BF16))
    shift = lax.axis_index("xy") * NVEC2 if place else 0
    home = iota((size, LANES), 1) == iota((size, LANES), 0) // count + shift
    line = [
        jnp.sum(jnp.where(home, summed[p * size : (p + 1) * size], 0.0), axis=0, keepdims=True)
        for p in range(2)
    ]
    both = jnp.where(iota((SUB, LANES), 0) % 2 == 0, line[0], line[1])
    for i in range(2 * dests // SUB):
        sent[i * SUB : (i + 1) * SUB] = both


def exchanged(x, step):
    rows = x.shape[0]
    if rows == 2 * step:
        return pltpu.roll(x, step, 0)
    up, down = pltpu.roll(x, rows - step, 0), pltpu.roll(x, step, 0)
    return jnp.where(iota(x.shape, 0) // step % 2 == 0, up, down)


def bottom_spread(v, spread, width):
    lane = iota(v.shape, 1)
    edge = width - NVEC2
    up = jnp.where(lane < edge, pltpu.roll(v, LANES - NVEC2, 1), pltpu.roll(v, edge, 1))
    down = jnp.where(lane >= NVEC2, pltpu.roll(v, NVEC2, 1), pltpu.roll(v, LANES - edge, 1))
    rows = jnp.concatenate([v, jnp.where(lane < width, up, 0.0), down], axis=0)
    return table_right(rows, spread[...], 3)


def bottom_products(near, image, held, cores):
    chunks = near.shape[1] // LANES
    stride = 6 * chunks
    for c in range(chunks):
        here = pl.ds(c * LANES, LANES)
        seen = [near[i * SUB : (i + 1) * SUB, here] for i in range(6)]
        turned = [exchanged(x, 1) for x in seen]
        for at, core in enumerate(cores):
            acc = [None, None]
            for n, rows in enumerate((seen, turned)):
                beside = exchanged(rows[core], 2)
                ways = [rows[core], beside, pltpu.roll(beside, 4, 0), rows[1 - core]]
                ways += [rows[2 + core], rows[4 + core]]
                for d, value in enumerate(ways):
                    block = held[at][pl.ds(d * chunks + c, SUB, stride=stride), :]
                    got = block * value
                    acc[n] = got if acc[n] is None else acc[n] + got
                row = (n * len(cores) + at) * SUB
                image[row : row + SUB, here] = acc[n]


def bottom_gather(image, gather, v):
    half = v.shape[0]
    total = table_right(image[: 2 * half], gather[...], 3)
    first, second = total[:half], total[half:]
    re = first - exchanged(first, 1)
    im = second + exchanged(second, 1)
    return bottom_shift * v + jnp.where(iota(v.shape, 0) % 2 == 0, re, im)


def whole_sum(x):
    return jnp.sum(jnp.sum(x, axis=1, keepdims=True), axis=0, keepdims=True)


def minimal_residual(r, f, s):
    sign = jnp.where(iota(r.shape, 0) % 2 == 0, 1.0, -1.0)
    r_turn, s_turn, f_turn = exchanged(r, 1), exchanged(s, 1), exchanged(f, 1)
    ff = whole_sum(f * f)
    ss = whole_sum(s * s)
    cross_re = whole_sum(f * s)
    cross_im = whole_sum(sign * f * s_turn)
    one_re = whole_sum(f * r)
    one_im = whole_sum(sign * f * r_turn)
    two_re = whole_sum(s * r)
    two_im = whole_sum(sign * s * r_turn)
    determinant = ff * ss - cross_re * cross_re - cross_im * cross_im
    a_re = (ss * one_re - (cross_re * two_re - cross_im * two_im)) / determinant
    a_im = (ss * one_im - (cross_re * two_im + cross_im * two_re)) / determinant
    b_re = (ff * two_re - (cross_re * one_re + cross_im * one_im)) / determinant
    b_im = (ff * two_im - (cross_re * one_im - cross_im * one_re)) / determinant
    return a_re * r + b_re * f - sign * (a_im * r_turn + b_im * f_turn)


def bottom_rows(nx, solution):
    rows = jnp.concatenate(
        [
            solution[0:4],
            solution[6:10],
            solution[0:2],
            solution[0:2],
            jnp.zeros((4, LANES), F32),
        ],
        axis=0,
    )
    x = lax.axis_index("xy")

    def turned(step):
        place = lax.rem(x + step + nx, nx)
        return pltpu.roll(rows, lax.rem(LANES - NVEC2 * place, LANES), 1)

    site = iota(rows.shape, 0) // 2
    near, far = turned(side_step("xy", 0)), turned(side_step("xy", 1))
    result = jnp.where(site == 4, near, jnp.where(site == 5, far, turned(0)))
    return jnp.where(iota(result.shape, 1) < NVEC2, result, 0.0)


def middle_step(counts, axes, blocks, rows, vectors, middle, read_block, fine, spinor, out, wide):
    per = LANES // blocks
    count = NVEC // per
    size = NVEC2 * count
    spread = one_hot(
        (iota((LANES, 2 * LANES), 0) == iota((LANES, 2 * LANES), 1) // count)
        & (iota((LANES, 2 * LANES), 1) < size)
    )
    coefs = table_right(rows, spread, 3)
    same = iota((NVEC, size), 1) % count == iota((NVEC, size), 0) % count
    guesses = []
    for n, ref in enumerate(vectors):
        skip = ref.shape[0] - 2 * size
        wide_vectors = jnp.concatenate(
            [ref[skip : skip + size], ref[skip + size : skip + 2 * size]], axis=1
        )
        left = jnp.concatenate(
            [jnp.where(same, coefs[2 * n + q : 2 * n + q + 1, :size], 0.0) for q in range(2)],
            axis=0,
        )
        made = product(left, wide_vectors)
        guesses.append(
            jnp.concatenate(
                [
                    made[:NVEC, :LANES] - made[NVEC:, LANES:],
                    made[:NVEC, LANES:] + made[NVEC:, :LANES],
                ],
                axis=0,
            )
        )
    own = guesses[0]
    near = [own]
    at = 1
    for c, axis in zip(counts, axes):
        near.extend(ahead_behind(guesses[at : at + c], axis))
        at += c
    aggregate = iota(own.shape, 1) % blocks
    near.append(
        jnp.where(
            aggregate == blocks - 1, pltpu.roll(own, blocks - 1, 1), pltpu.roll(own, LANES - 1, 1)
        )
    )
    near.append(
        jnp.where(aggregate == 0, pltpu.roll(own, LANES - blocks + 1, 1), pltpu.roll(own, 1, 1))
    )
    count_blocks = size // NVEC
    sums = [[None, None] for _ in range(count_blocks)]
    for d, value in enumerate(near):
        re, im = value[:NVEC], value[NVEC:]
        for block in range(count_blocks):
            m_re, m_im = [read_block(p, d, block) for p in range(2)]
            got = [m_re * re - m_im * im, m_re * im + m_im * re]
            sums[block] = [g if a is None else a + g for a, g in zip(sums[block], got)]
    made_re, made_im = [], []
    for block in range(count_blocks):
        acc_re, acc_im = sums[block]
        row = iota((NVEC, LANES), 0) + block * NVEC
        at_home = (row % count) * per + iota((NVEC, LANES), 1) // blocks == row // count
        keep = 1.0 - middle_damping * middle_shift
        made_re.append(jnp.where(at_home, keep * own[:NVEC], 0.0) - middle_damping * acc_re)
        made_im.append(jnp.where(at_home, keep * own[NVEC:], 0.0) - middle_damping * acc_im)
    made = jnp.concatenate(
        [jnp.concatenate(made_re, axis=0), jnp.concatenate(made_im, axis=0)], axis=1
    )
    row_sum = one_hot(iota((NVEC, size), 1) // count == iota((NVEC, size), 0))
    summed = table_left(row_sum, made)
    summed = jnp.concatenate([summed[:, :LANES], summed[:, LANES:]], axis=0)
    lane_sum = one_hot(
        iota((LANES, LANES), 0) % blocks == iota((LANES, LANES), 1) % blocks
    )
    update = table_right(summed, lane_sum) + middle_damping * middle[...]
    lift = one_hot(iota((LANES, LANES), 0) == iota((LANES, LANES), 1) // BY)
    lifted = jnp.dot(update.astype(BF16), lift, preferred_element_type=F32)
    u_re, u_im = lifted[:NVEC], lifted[NVEC:]
    wide[...] = fine[...].astype(F32)
    sum_re, sum_im = [], []
    for i in range(HALF):
        re, im = strided_vectors(wide, i)
        sum_re.append(jnp.sum(re * u_re - im * u_im, axis=0, keepdims=True))
        sum_im.append(jnp.sum(re * u_im + im * u_re, axis=0, keepdims=True))
    out[...] = spinor[...] + jnp.concatenate(sum_re + sum_im, axis=0)


def start_kernel(shape, received, held, spread, gather, right, near, own, image):
    nt, nz, nx = shape
    ta, gz = lax.axis_index("ta"), lax.axis_index("gz")
    total = received.shape[0]
    row, col = iota((2 * SUB, total), 0), iota((2 * SUB, total), 1)
    line = (ta ^ (row // 2 % nt)) * nz + (gz ^ (row // SUB))
    fold = one_hot((col // (2 * nx) == line) & (col % 2 == row % 2))
    r = table_left(fold, received[...], 3)
    right[...] = r
    near[...] = bottom_spread(r, spread, nx * NVEC2)
    bottom_products(near, image, (held,), (0,))
    own[...] = bottom_gather(image, gather, r[:SUB])


def third_kernel(counts, axes, blocks, shape, right, *refs):
    passing = pltpu.make_async_copy(refs[0], refs[-5], refs[-1])
    passing.start()
    refs = refs[1:-1]
    n_sites = 1 + sum(counts)
    first_near, own, refs = refs[0], refs[1], refs[2:]
    held, spread, gather, matrix, refs = refs[:2], refs[2], refs[3], refs[4], refs[5:]
    vectors, refs = refs[:n_sites], refs[n_sites:]
    middle, fine, spinor, out, _, near, image, wide = refs
    nx = shape[2]
    r = right[...]
    bottom_products(first_near, image, (held[1],), (1,))
    f = jnp.concatenate([own[...], bottom_gather(image, gather, r[SUB:])], axis=0)
    near[...] = bottom_spread(f, spread, nx * NVEC2)
    bottom_products(near, image, held, (0, 1))
    s = bottom_gather(image, gather, f)
    rows = bottom_rows(nx, minimal_residual(r, f, s))
    size = NVEC * NVEC * blocks // LANES

    def read_block(p, d, block):
        return matrix[pl.ds((p * 9 + d) * size + block * NVEC, NVEC), :]

    middle_step(
        counts, axes, blocks, rows, vectors, middle, read_block, fine, spinor, out, wide
    )
    passing.wait()


def fourth_kernel(counts, axes, blocks, rows, *refs):
    n_sites = 1 + sum(counts)
    matrix, refs = refs[0], refs[1:]
    vectors, refs = refs[:n_sites], refs[n_sites:]
    middle, fine, spinor, out, wide = refs
    size = NVEC * NVEC * blocks // LANES

    def read_block(p, d, block):
        return matrix[pl.ds((p * 9 + d) * size + block * NVEC, NVEC), :]

    middle_step(
        counts, axes, blocks, rows[...], vectors, middle, read_block, fine, spinor, out, wide
    )


def vmem():
    return pl.BlockSpec(memory_space=pltpu.VMEM)


def anywhere():
    return pl.BlockSpec(memory_space=pl.ANY)


def shape_of(*dims):
    return jax.ShapeDtypeStruct(dims, F32)


def params(mib):
    return pltpu.CompilerParams(vmem_limit_bytes=mib * 2**20)


def line_solve(right, bottom_blocks):
    split = bottom_blocks.reshape((2, 7, -1, NVEC2, NVEC2))
    line = lax.all_gather(right, "xy", axis=1, tiled=False)

    def turned(v, axis, step):
        n = lax.axis_size(axis)
        return lax.ppermute(v, axis, [((i + step) % n, i) for i in range(n)])

    def product(blocks, v):
        return jnp.einsum("dxjk,dxk->xj", blocks, v, precision=HIGHEST)

    def apply(v):
        near = [v, turned(v, "ta", 1), turned(v, "ta", -1), turned(v, "gz", 1), turned(v, "gz", -1)]
        near = jnp.stack(near + [jnp.roll(v, -1, 1), jnp.roll(v, 1, 1)], axis=1)
        re = product(split[0], near[0]) - product(split[1], near[1])
        im = product(split[0], near[1]) + product(split[1], near[0])
        return bottom_shift * v + jnp.stack([re, im])

    first = apply(line)
    second = apply(first)

    def inner(u, w):
        return [jnp.sum(u[0] * w[0] + u[1] * w[1]), jnp.sum(u[0] * w[1] - u[1] * w[0])]

    sums = inner(first, first)[:1] + inner(second, second)[:1] + inner(first, second)
    sums = sums + inner(first, line) + inner(second, line)
    ff, ss, cr, ci, pr, pi, qr, qi = lax.psum(jnp.stack(sums), ("ta", "gz"))
    det = ff * ss - cr * cr - ci * ci
    a_re = (ss * pr - (cr * qr - ci * qi)) / det
    a_im = (ss * pi - (cr * qi + ci * qr)) / det
    b_re = (ff * qr - (cr * pr + ci * pi)) / det
    b_im = (ff * qi - (cr * pi - ci * pr)) / det

    def scaled(re, im, v):
        return jnp.stack([re * v[0] - im * v[1], re * v[1] + im * v[0]])

    solved = scaled(a_re, a_im, line) + scaled(b_re, b_im, first)
    return lax.dynamic_index_in_dim(solved, lax.axis_index("xy"), 1, keepdims=False)


def shards(source_field, gauge_links, fine_vectors, middle_blocks, middle_vectors, bottom_blocks):
    axes = ("ta", "gz", "xy")
    shape = tuple(lax.axis_size(a) for a in axes)
    nt, nz, nx = shape
    devices = nt * nz * nx
    blocks = source_field.shape[-1] // BY
    source = source_field.reshape(SPINOR, LANES)
    gauge = gauge_links.reshape(-1, LANES)
    fine = jnp.transpose(fine_vectors, (0, 1, 3, 4, 5, 6, 2, 7)).reshape(-1, LANES)
    matrix = middle_blocks.reshape(-1, LANES)
    vectors = middle_vectors.reshape(-1, LANES)
    size = vectors.shape[0]
    project, rebuild = fine_tables()
    counts = [len(pairings(n)) for n in shape]
    gathered = nt == 4 and nz == 2 and 2 < nx and nx % 2 == 0 and nx * NVEC2 <= LANES

    halos = neighbours(source, axes)
    flat = [a for pair in halos for a in pair]
    loads = [source, gauge, fine, project, rebuild, vectors]
    shapes = [jax.ShapeDtypeStruct(a.shape, a.dtype) for a in loads]
    scratch = []
    depth = 0
    if gathered:
        depth = bottom_blocks.shape[-1] * 12 // LANES
        loads.append(bottom_blocks.reshape(1, -1))
        shapes.append(shape_of(depth, LANES))
        scratch.append(pltpu.VMEM(loads[-1].shape, F32))
    loaded = pl.pallas_call(
        functools.partial(load_kernel, gathered),
        out_shape=tuple(shapes),
        in_specs=[pl.BlockSpec(memory_space=pltpu.HBM)] * len(loads),
        out_specs=(vmem(),) * len(shapes),
        scratch_shapes=scratch + [pltpu.SemaphoreType.DMA((len(loads),))],
        compiler_params=params(4),
    )(*[pltpu.with_memory_space_constraint(a, pltpu.HBM) for a in loads])
    source, gauge, fine, project, rebuild, mine = loaded[:6]
    if gathered:
        line = loaded[6]
        beside = lax.ppermute(line, "ta", [(i, i ^ 1) for i in range(nt)])
        pair = jnp.concatenate([line, beside])
    spinor, payload = pl.pallas_call(
        functools.partial(first_kernel, counts, axes),
        out_shape=(shape_of(SPINOR, LANES), shape_of(SPINOR + size, LANES)),
        in_specs=[vmem()] * (len(flat) + 5),
        out_specs=(vmem(), vmem()),
        compiler_params=params(8),
    )(source, *flat, gauge, mine, project, rebuild)

    alone = (("ta", 0), ("xy", 1)) if gathered else ()
    near = neighbours(lambda axis, i: spinor if (axis, i) in alone else payload, axes)
    flat_near = [a for pair in near for a in pair]
    near_vectors = list(flat_near)
    if gathered:
        other = lax.ppermute(pair, "ta", [(i, i ^ 2) for i in range(nt)])
        near_vectors[0] = lax.ppermute(vectors, "ta", pairings(nt)[0])
        near_vectors[-1] = lax.ppermute(vectors, "xy", pairings(nx)[1])
    dests = devices if gathered else SUB
    residual, middle, sent = pl.pallas_call(
        functools.partial(second_kernel, counts, axes, blocks, gathered, dests),
        out_shape=(shape_of(SPINOR, LANES), shape_of(2 * NVEC, LANES), shape_of(2 * dests, LANES)),
        in_specs=[vmem()] * (7 + len(flat_near)),
        out_specs=(vmem(), vmem(), vmem()),
        scratch_shapes=[pltpu.VMEM(fine.shape, F32)],
        compiler_params=params(8),
    )(source, spinor, *flat_near, gauge, fine, mine, project, rebuild)

    if gathered:
        received = lax.all_to_all(sent.reshape(devices, 2, LANES), axes, 0, 0)
        received = received.reshape(2 * devices, LANES)
        received, pair, other = lax.optimization_barrier((received, pair, other))
        held = jnp.concatenate([pair, other])
        held = [held, lax.ppermute(held, "gz", pairings(nz)[0])]
        lane = np.arange(nx * NVEC2 * NVEC2)
        k_lane = np.arange(LANES)[:, None]
        spread = k_lane == (lane // (NVEC2 * NVEC2) * NVEC2 + lane % NVEC2)[None]
        gather = k_lane.T == (lane // NVEC2)[:, None]
        spread, gather = jnp.asarray(spread, BF16), jnp.asarray(gather, BF16)
        right, first_near, own = pl.pallas_call(
            functools.partial(start_kernel, shape),
            out_shape=(
                shape_of(2 * SUB, LANES),
                shape_of(6 * SUB, lane.size),
                shape_of(SUB, LANES),
            ),
            in_specs=[vmem()] * 4,
            out_specs=(vmem(),) * 3,
            scratch_shapes=[pltpu.VMEM((2 * SUB, lane.size), F32)],
            compiler_params=params(8),
        )(received, held[0], spread, gather)
        solution, residual = pl.pallas_call(
            functools.partial(third_kernel, counts, axes, blocks, shape),
            out_shape=(shape_of(SPINOR, LANES), shape_of(SPINOR, LANES)),
            in_specs=[vmem()] * (13 + len(flat_near)),
            out_specs=(vmem(), anywhere()),
            scratch_shapes=[
                pltpu.VMEM((6 * SUB, lane.size), F32),
                pltpu.VMEM((4 * SUB, lane.size), F32),
                pltpu.VMEM(fine.shape, F32),
                pltpu.SemaphoreType.DMA,
            ],
            compiler_params=params(8),
        )(right, residual, first_near, own, *held, spread, gather, matrix, mine, *near_vectors, middle, fine, spinor)
    else:
        solved = line_solve(sent[:2, :NVEC2], bottom_blocks)
        solved = jnp.pad(solved, ((0, 0), (0, LANES - NVEC2)))
        rows = [solved] + [a for pair in neighbours(solved, axes) for a in pair]
        rows = jnp.concatenate(rows)
        rows = jnp.pad(rows, ((0, 2 * SUB - rows.shape[0]), (0, 0)))
        solution = pl.pallas_call(
            functools.partial(fourth_kernel, counts, axes, blocks),
            out_shape=shape_of(SPINOR, LANES),
            in_specs=[vmem()] * (6 + len(flat_near)),
            out_specs=vmem(),
            scratch_shapes=[pltpu.VMEM(fine.shape, F32)],
            compiler_params=params(16),
        )(rows, matrix, mine, *near_vectors, middle, fine, spinor)
    return solution.reshape(source_field.shape), residual.reshape(source_field.shape)


def solution(mesh):
    return jax.shard_map(
        shards,
        mesh=mesh,
        in_specs=(
            P(None, None, None, "ta", "gz", "xy", None),
            P(None, None, None, None, "ta", "gz", "xy", None),
            P(None, None, None, None, "ta", "gz", "xy", None),
            P(None, None, None, "ta", "gz", "xy", None),
            P(None, None, "ta", "gz", "xy", None),
            P(None, None, "ta", "gz", None),
        ),
        out_specs=(
            P(None, None, None, "ta", "gz", "xy", None),
            P(None, None, None, "ta", "gz", "xy", None),
        ),
        check_vma=False,
    )
```

```python
import functools

import jax
import jax.numpy as jnp
import numpy as np
from jax import lax
from jax.experimental import pallas as pl
from jax.experimental.pallas import tpu as pltpu
from jax.sharding import PartitionSpec as P


BY = 4
NVEC = 24
NVEC2 = 24
SPINOR = 24
HALF = 12
LANES = 128
SUB = 8

quark_mass = 0.1
twist_mass = 0.1
fine_damping = 0.8
middle_damping = 0.4
middle_shift = 2.0
bottom_shift = 2.0
gamma = np.array(
    [
        [[0, 0, 1, 0], [0, 0, 0, 1], [1, 0, 0, 0], [0, 1, 0, 0]],
        [[0, 0, 1j, 0], [0, 0, 0, -1j], [-1j, 0, 0, 0], [0, 1j, 0, 0]],
        [[0, 0, 0, 1j], [0, 0, 1j, 0], [0, -1j, 0, 0], [-1j, 0, 0, 0]],
        [[0, 0, 0, -1], [0, 0, 1, 0], [0, 1, 0, 0], [-1, 0, 0, 0]],
    ],
    np.complex64,
)
HIGHEST = lax.Precision.HIGHEST
F32 = jnp.float32
BF16 = jnp.bfloat16


def real_form(matrix):
    return np.block([[matrix.real, -matrix.imag], [matrix.imag, matrix.real]])


def fine_tables():
    color = np.eye(3)
    project = np.zeros((2, 2, 3, 8, 8, SPINOR))
    rebuild = np.zeros((SPINOR, 2, 2, 3, 8))
    for m in range(4):
        for back in range(2):
            sign = -1.0 if back else 1.0
            way = 2 * m + back
            upper = np.eye(4)[:2] - sign * gamma[m][:2]
            project[:, :, :, way, way] = real_form(np.kron(upper, color)).reshape(2, 2, 3, SPINOR)
            lower = np.concatenate([np.eye(2), -sign * gamma[m][2:, :2]])
            rebuild[..., way] = real_form(np.kron(lower, color)).reshape(SPINOR, 2, 2, 3)
    project = project.reshape(HALF * 8, 8 * SPINOR)
    rebuild = rebuild.reshape(SPINOR, HALF * 8)
    return [jnp.asarray(t, BF16) for t in (project, rebuild)]


def twisted(x, straight, crossed):
    count = x.shape[0] // SPINOR
    pieces = []
    for i in range(count):
        pieces += [x[i * SPINOR + HALF : (i + 1) * SPINOR], x[i * SPINOR : i * SPINOR + HALF]]
    other = jnp.concatenate(pieces, axis=0)
    row = iota(x.shape, 0) % SPINOR
    sign = jnp.where((row % HALF < HALF // 2) != (row < HALF), crossed, -crossed)
    return straight * x + sign * other


def inverse_of(x, scale):
    mass = 4.0 + quark_mass
    norm = mass * mass + twist_mass * twist_mass
    return twisted(x, scale * mass / norm, -scale * twist_mass / norm)


def pairings(n):
    if n % 2:
        return [[((i + 1) % n, i) for i in range(n)], [(i, (i + 1) % n) for i in range(n)]]
    near = [(i, i ^ 1) for i in range(n)]
    far = [(i, (i + 1) % n if i % 2 else (i - 1) % n) for i in range(n)]
    return [near] if n == 2 else [near, far]


def neighbours(array, axes):
    found = []
    for axis in axes:
        pairs = pairings(lax.axis_size(axis))
        found.append(
            [
                lax.ppermute(array(axis, i) if callable(array) else array, axis, p)
                for i, p in enumerate(pairs)
            ]
        )
    return found


def load_kernel(has_line, *refs):
    sems = refs[-1]
    count = sems.shape[0]
    ins, outs = refs[:count], list(refs[count : 2 * count])
    if has_line:
        out, outs[-1] = outs[-1], refs[-2]
    copies = [pltpu.make_async_copy(ins[i], outs[i], sems.at[i]) for i in range(count)]
    for copy in reversed(copies):
        copy.start()
    if has_line:
        copies[-1].wait()
        source = outs[-1]
        chunks = out.shape[0] // 12
        even = lax.axis_index("ta") % 2 == 0
        for p in range(2):
            way = [
                source[:, (p * 7 + d) * chunks * LANES : (p * 7 + d + 1) * chunks * LANES]
                for d in range(7)
            ]
            ahead, behind = way[1], way[2]
            ways = [way[0], jnp.where(even, ahead, behind), jnp.where(even, behind, ahead)]
            ways += [way[3] + way[4], way[5], way[6]]
            for d, value in enumerate(ways):
                for c in range(chunks):
                    row = (p * 6 + d) * chunks + c
                    out[row : row + 1] = value[:, c * LANES : (c + 1) * LANES]
        copies = copies[:-1]
    for copy in copies:
        copy.wait()


def side_step(axis, which):
    n = lax.axis_size(axis)
    ahead = 1 if which == 0 else -1
    if n % 2:
        return ahead
    return ahead * (1 - 2 * (lax.axis_index(axis) % 2))


def ahead_behind(pair, axis):
    if len(pair) == 1:
        return pair[0], pair[0]
    n = lax.axis_size(axis)
    if n % 2:
        return pair[0], pair[1]
    even = lax.axis_index(axis) % 2 == 0
    return jnp.where(even, pair[0], pair[1]), jnp.where(even, pair[1], pair[0])


def parts(x, count):
    found = []
    for _ in range(count):
        found.append(x.astype(BF16))
        x = x - found[-1].astype(F32)
    return found


def table_left(table, x, count=2):
    n = x.shape[1]
    out = jnp.dot(table, jnp.concatenate(parts(x, count), axis=1), preferred_element_type=F32)
    return sum(out[:, i * n : (i + 1) * n] for i in range(count))


def table_right(x, table, count=2):
    m = x.shape[0]
    out = jnp.dot(jnp.concatenate(parts(x, count), axis=0), table, preferred_element_type=F32)
    return sum(out[i * m : (i + 1) * m] for i in range(count))


def product(a, b_high, b_low):
    m = a.shape[0]
    a_high, a_low = parts(a, 2)
    out = jnp.dot(jnp.concatenate([a_high, a_low], axis=0), b_high, preferred_element_type=F32)
    return out[:m] + out[m:] + jnp.dot(a_high, b_low, preferred_element_type=F32)


def iota(shape, dim):
    return lax.broadcasted_iota(jnp.int32, shape, dim)


def one_hot(condition, dtype=BF16):
    return jnp.where(condition, 1.0, 0.0).astype(dtype)


def hopping(spinor, halos, gauge, project, rebuild, axes, change=None):
    seen = []
    for pair, axis in zip(halos, axes):
        seen.extend(ahead_behind(pair, axis))
    seen.append(pltpu.roll(spinor, LANES - 1, 1))
    seen.append(pltpu.roll(spinor, 1, 1))
    seen = jnp.concatenate(seen, axis=0)
    half = table_left(project, seen if change is None else change(seen))
    rows = [[[None] * 3 for _ in range(2)] for _ in range(2)]
    for a in range(3):
        for b in range(3):
            link = [gauge[pl.ds(p * 72 + a * 3 + b, 8, stride=9), :] for p in range(2)]
            for s in range(2):
                re = half[(s * 3 + b) * 8 : (s * 3 + b) * 8 + 8]
                im = half[(6 + s * 3 + b) * 8 : (6 + s * 3 + b) * 8 + 8]
                out_re = link[0] * re - link[1] * im
                out_im = link[0] * im + link[1] * re
                for p, value in ((0, out_re), (1, out_im)):
                    old = rows[p][s][a]
                    rows[p][s][a] = value if old is None else old + value
    rows = [rows[p][s][a] for p in range(2) for s in range(2) for a in range(3)]
    return table_left(rebuild, jnp.concatenate(rows, axis=0))


def first_kernel(counts, axes, *refs):
    source, refs = refs[0], refs[1:]
    halos, at = [], 0
    for count in counts:
        halos.append([r[:SPINOR] for r in refs[at : at + count]])
        at += count
    gauge, vectors, project, rebuild, alone, out = refs[at:]
    value = source[...]
    start = functools.partial(inverse_of, scale=fine_damping)
    hop = hopping(value, halos, gauge, project[...], rebuild[...], axes, start)
    result = inverse_of(
        fine_damping * (2.0 - fine_damping) * value + 0.5 * fine_damping * hop, 1.0
    )
    alone[...] = result
    out[:SPINOR] = result
    size = out.shape[0] - SPINOR
    out[SPINOR:] = vectors[pl.ds(vectors.shape[0] - size, size), :]


def strided_vectors(fine, i):
    row = (i % 3) * 4 + i // 3
    return [fine[pl.ds(p * NVEC * HALF + row, NVEC, stride=HALF), :] for p in range(2)]


def second_kernel(counts, axes, blocks, together, *refs):
    source, own, refs = refs[0], refs[1], refs[2:]
    halos, at = [], 0
    for count in counts:
        halos.append([r[:SPINOR] for r in refs[at : at + count]])
        at += count
    gauge, fine, vectors, project, rebuild, out, middle, sent, wide = refs[at:]
    spinor = own[...]
    hop = hopping(spinor, halos, gauge, project[...], rebuild[...], axes)
    residual = source[...] - twisted(spinor, 4.0 + quark_mass, twist_mass) + 0.5 * hop
    out[...] = residual
    low = residual.astype(BF16).astype(F32)
    wide[...] = fine[...].astype(F32)
    sum_re = jnp.zeros((NVEC, LANES), F32)
    sum_im = jnp.zeros((NVEC, LANES), F32)
    for i in range(HALF):
        re, im = strided_vectors(wide, i)
        low_re, low_im = low[i : i + 1], low[HALF + i : HALF + i + 1]
        sum_re = sum_re + re * low_re + im * low_im
        sum_im = sum_im + re * low_im - im * low_re
    group = iota((LANES, LANES), 1) % blocks == iota((LANES, LANES), 0) // BY
    right = table_right(jnp.concatenate([sum_re, sum_im], axis=0), one_hot(group))
    middle[...] = right
    per = LANES // blocks
    count = NVEC // per
    keep = iota((NVEC, LANES), 1) // blocks == iota((NVEC, LANES), 0) % per
    pick = one_hot(iota((NVEC, NVEC), 1) // per == iota((NVEC, NVEC), 0) % count)
    kept = [jnp.where(keep, right[p * NVEC : (p + 1) * NVEC], 0.0) for p in range(2)]
    pattern = table_left(pick, jnp.concatenate(kept, axis=1))
    pat_re, pat_im = pattern[:, :LANES], pattern[:, LANES:]
    size = NVEC2 * count
    skip = vectors.shape[0] - 2 * size
    made_re, made_im = [], []
    for block in range(size // NVEC):
        re = vectors[pl.ds(skip + block * NVEC, NVEC), :]
        im = vectors[pl.ds(skip + size + block * NVEC, NVEC), :]
        made_re.append(re * pat_re + im * pat_im)
        made_im.append(re * pat_im - im * pat_re)
    made = jnp.concatenate(made_re + made_im, axis=0)
    summed = table_right(made, jnp.ones((LANES, LANES), BF16))
    line = []
    for p in range(2):
        home = iota((size, LANES), 0) // count + (p * NVEC2 if together else 0)
        kept = jnp.where(iota((size, LANES), 1) == home, summed[p * size : (p + 1) * size], 0.0)
        line.append(jnp.sum(kept, axis=0, keepdims=True))
    if together:
        both = jnp.broadcast_to(line[0] + line[1], (SUB, LANES))
    else:
        both = jnp.where(iota((SUB, LANES), 0) % 2 == 0, line[0], line[1])
    for i in range(sent.shape[0] // SUB):
        sent[i * SUB : (i + 1) * SUB] = both


def exchanged(x, step):
    rows = x.shape[0]
    if rows == 2 * step:
        return pltpu.roll(x, step, 0)
    if rows == SUB:
        return jnp.take_along_axis(x, iota(x.shape, 0) ^ step, axis=0)
    up, down = pltpu.roll(x, rows - step, 0), pltpu.roll(x, step, 0)
    return jnp.where(iota(x.shape, 0) // step % 2 == 0, up, down)


def bottom_spread(v, spread, width):
    lane = iota(v.shape, 1)
    edge = width - NVEC2
    up = jnp.where(lane < edge, pltpu.roll(v, LANES - NVEC2, 1), pltpu.roll(v, edge, 1))
    down = jnp.where(lane >= NVEC2, pltpu.roll(v, NVEC2, 1), pltpu.roll(v, LANES - edge, 1))
    rows = jnp.concatenate([v, jnp.where(lane < width, up, 0.0), down], axis=0)
    return table_right(rows, spread[...], 3)


def bottom_products(near, image, held, cores):
    chunks = near.shape[1] // LANES
    stride = 6 * chunks
    for c in range(chunks):
        here = pl.ds(c * LANES, LANES)
        seen = [near[i * SUB : (i + 1) * SUB, here] for i in range(6)]
        turned = [exchanged(x, 1) for x in seen]
        for at, core in enumerate(cores):
            acc = [None, None]
            for n, rows in enumerate((seen, turned)):
                beside = exchanged(rows[core], 2)
                ways = [rows[core], beside, pltpu.roll(beside, 4, 0), rows[1 - core]]
                ways += [rows[2 + core], rows[4 + core]]
                for d, value in enumerate(ways):
                    block = held[at][pl.ds(d * chunks + c, SUB, stride=stride), :]
                    got = block * value
                    acc[n] = got if acc[n] is None else acc[n] + got
                row = (n * len(cores) + at) * SUB
                image[row : row + SUB, here] = acc[n]


def bottom_gather(image, gather, v):
    half = v.shape[0]
    total = table_right(image[: 2 * half], gather[...], 3)
    first, second = total[:half], total[half:]
    re = first - exchanged(first, 1)
    im = second + exchanged(second, 1)
    return bottom_shift * v + jnp.where(iota(v.shape, 0) % 2 == 0, re, im)


def whole_sum(x):
    return jnp.sum(jnp.sum(x, axis=1, keepdims=True), axis=0, keepdims=True)


def minimal_residual(r, f, s):
    sign = jnp.where(iota(r.shape, 0) % 2 == 0, 1.0, -1.0)
    r_turn, s_turn, f_turn = exchanged(r, 1), exchanged(s, 1), exchanged(f, 1)
    ff = whole_sum(f * f)
    ss = whole_sum(s * s)
    cross_re = whole_sum(f * s)
    cross_im = whole_sum(sign * f * s_turn)
    one_re = whole_sum(f * r)
    one_im = whole_sum(sign * f * r_turn)
    two_re = whole_sum(s * r)
    two_im = whole_sum(sign * s * r_turn)
    determinant = ff * ss - cross_re * cross_re - cross_im * cross_im
    a_re = (ss * one_re - (cross_re * two_re - cross_im * two_im)) / determinant
    a_im = (ss * one_im - (cross_re * two_im + cross_im * two_re)) / determinant
    b_re = (ff * two_re - (cross_re * one_re + cross_im * one_im)) / determinant
    b_im = (ff * two_im - (cross_re * one_im - cross_im * one_re)) / determinant
    return a_re * r + b_re * f - sign * (a_im * r_turn + b_im * f_turn)


def bottom_rows(nx, solution):
    rows = jnp.concatenate(
        [
            solution[0:4],
            solution[6:10],
            solution[0:2],
            solution[0:2],
            jnp.zeros((4, LANES), F32),
        ],
        axis=0,
    )
    x = lax.axis_index("xy")

    def turned(step):
        place = lax.rem(x + step + nx, nx)
        return pltpu.roll(rows, lax.rem(LANES - NVEC2 * place, LANES), 1)

    site = iota(rows.shape, 0) // 2
    near, far = turned(side_step("xy", 0)), turned(side_step("xy", 1))
    result = jnp.where(site == 4, near, jnp.where(site == 5, far, turned(0)))
    return jnp.where(iota(result.shape, 1) < NVEC2, result, 0.0)


def vector_parts(ref, size):
    skip = ref.shape[0] - 2 * size
    both = jnp.concatenate(
        [ref[skip : skip + size], ref[skip + size : skip + 2 * size]], axis=1
    )
    return parts(both, 2)


def middle_step(counts, axes, blocks, rows, pairs, middle, read_block, wide, spinor, out):
    per = LANES // blocks
    count = NVEC // per
    size = NVEC2 * count
    spread = one_hot(
        (iota((LANES, 2 * LANES), 0) == iota((LANES, 2 * LANES), 1) // count)
        & (iota((LANES, 2 * LANES), 1) < size)
    )
    coefs = table_right(rows, spread, 3)
    same = iota((NVEC, size), 1) % count == iota((NVEC, size), 0) % count
    guesses = []
    for n, pair in enumerate(pairs):
        left = jnp.concatenate(
            [jnp.where(same, coefs[2 * n + q : 2 * n + q + 1, :size], 0.0) for q in range(2)],
            axis=0,
        )
        made = product(left, *pair)
        guesses.append(
            jnp.concatenate(
                [
                    made[:NVEC, :LANES] - made[NVEC:, LANES:],
                    made[:NVEC, LANES:] + made[NVEC:, :LANES],
                ],
                axis=0,
            )
        )
    own = guesses[0]
    near = [own]
    at = 1
    for c, axis in zip(counts, axes):
        near.extend(ahead_behind(guesses[at : at + c], axis))
        at += c
    aggregate = iota(own.shape, 1) % blocks
    near.append(
        jnp.where(
            aggregate == blocks - 1, pltpu.roll(own, blocks - 1, 1), pltpu.roll(own, LANES - 1, 1)
        )
    )
    near.append(
        jnp.where(aggregate == 0, pltpu.roll(own, LANES - blocks + 1, 1), pltpu.roll(own, 1, 1))
    )
    count_blocks = size // NVEC
    sums = [[None, None] for _ in range(count_blocks)]
    for d, value in enumerate(near):
        re, im = value[:NVEC], value[NVEC:]
        for block in range(count_blocks):
            m_re, m_im = [read_block(p, d, block) for p in range(2)]
            got = [m_re * re - m_im * im, m_re * im + m_im * re]
            sums[block] = [g if a is None else a + g for a, g in zip(sums[block], got)]
    made_re, made_im = [], []
    for block in range(count_blocks):
        acc_re, acc_im = sums[block]
        row = iota((NVEC, LANES), 0) + block * NVEC
        at_home = (row % count) * per + iota((NVEC, LANES), 1) // blocks == row // count
        keep = 1.0 - middle_damping * middle_shift
        made_re.append(jnp.where(at_home, keep * own[:NVEC], 0.0) - middle_damping * acc_re)
        made_im.append(jnp.where(at_home, keep * own[NVEC:], 0.0) - middle_damping * acc_im)
    made = jnp.concatenate(
        [jnp.concatenate(made_re, axis=0), jnp.concatenate(made_im, axis=0)], axis=1
    )
    row_sum = one_hot(iota((NVEC, size), 1) // count == iota((NVEC, size), 0))
    summed = table_left(row_sum, made)
    summed = jnp.concatenate([summed[:, :LANES], summed[:, LANES:]], axis=0)
    lane_sum = one_hot(
        iota((LANES, LANES), 0) % blocks == iota((LANES, LANES), 1) % blocks
    )
    update = table_right(summed, lane_sum) + middle_damping * middle[...]
    lift = one_hot(iota((LANES, LANES), 0) == iota((LANES, LANES), 1) // BY)
    lifted = jnp.dot(update.astype(BF16), lift, preferred_element_type=F32)
    u_re, u_im = lifted[:NVEC], lifted[NVEC:]
    sum_re, sum_im = [], []
    for i in range(HALF):
        re, im = strided_vectors(wide, i)
        sum_re.append(jnp.sum(re * u_re - im * u_im, axis=0, keepdims=True))
        sum_im.append(jnp.sum(re * u_im + im * u_re, axis=0, keepdims=True))
    out[...] = spinor[...] + jnp.concatenate(sum_re + sum_im, axis=0)


def start_kernel(shape, received, held, spread, gather, right, near, own, image):
    nt, nz, nx = shape
    ta, gz = lax.axis_index("ta"), lax.axis_index("gz")
    total, rows = received.shape[0], 2 * SUB
    row, col = iota((nx * rows, total), 0), iota((nx * rows, total), 1)
    line = (ta ^ (row % rows // 2 % nt)) * nz + (gz ^ (row % rows // SUB))
    fold = one_hot(col == line * nx + row // rows)
    found = table_left(fold, received[...], 3)
    lane, part = iota((rows, LANES), 1), iota((rows, LANES), 0) % 2
    r = jnp.zeros((rows, LANES), F32)
    for x in range(nx):
        block = found[x * rows : (x + 1) * rows]
        turned = [pltpu.roll(block, ((x - q) * NVEC2) % LANES, 1) for q in range(2)]
        r = jnp.where(lane // NVEC2 == x, jnp.where(part == 0, turned[0], turned[1]), r)
    right[...] = r
    near[...] = bottom_spread(r, spread, nx * NVEC2)
    bottom_products(near, image, (held,), (0,))
    own[...] = bottom_gather(image, gather, r[:SUB])


def third_kernel(counts, axes, blocks, shape, right, *refs):
    passing = pltpu.make_async_copy(refs[0], refs[-5], refs[-1])
    passing.start()
    refs = refs[1:-1]
    n_sites = 1 + sum(counts)
    first_near, own, refs = refs[0], refs[1], refs[2:]
    held, spread, gather, matrix, refs = refs[:2], refs[2], refs[3], refs[4], refs[5:]
    vectors, refs = refs[:n_sites], refs[n_sites:]
    middle, fine, spinor, out, _, near, image, wide = refs
    wide[...] = fine[...].astype(F32)
    nx = shape[2]
    r = right[...]
    bottom_products(first_near, image, (held[1],), (1,))
    f = jnp.concatenate([own[...], bottom_gather(image, gather, r[SUB:])], axis=0)
    near[...] = bottom_spread(f, spread, nx * NVEC2)
    bottom_products(near, image, held, (0, 1))
    s = bottom_gather(image, gather, f)
    rows = bottom_rows(nx, minimal_residual(r, f, s))
    size = NVEC * NVEC * blocks // LANES

    def read_block(p, d, block):
        return matrix[pl.ds((p * 9 + d) * size + block * NVEC, NVEC), :]

    pairs = [vector_parts(ref, NVEC2 * NVEC * blocks // LANES) for ref in vectors]
    middle_step(counts, axes, blocks, rows, pairs, middle, read_block, wide, spinor, out)
    passing.wait()


def fourth_kernel(counts, axes, blocks, rows, *refs):
    n_sites = 1 + sum(counts)
    matrix, refs = refs[0], refs[1:]
    vectors, refs = refs[:n_sites], refs[n_sites:]
    middle, fine, spinor, out, wide = refs
    size = NVEC * NVEC * blocks // LANES

    def read_block(p, d, block):
        return matrix[pl.ds((p * 9 + d) * size + block * NVEC, NVEC), :]

    wide[...] = fine[...].astype(F32)
    pairs = [vector_parts(ref, NVEC2 * NVEC * blocks // LANES) for ref in vectors]
    middle_step(counts, axes, blocks, rows[...], pairs, middle, read_block, wide, spinor, out)


def vmem():
    return pl.BlockSpec(memory_space=pltpu.VMEM)


def anywhere():
    return pl.BlockSpec(memory_space=pl.ANY)


def shape_of(*dims):
    return jax.ShapeDtypeStruct(dims, F32)


def params(mib):
    return pltpu.CompilerParams(vmem_limit_bytes=mib * 2**20)


def line_solve(right, bottom_blocks):
    split = bottom_blocks.reshape((2, 7, -1, NVEC2, NVEC2))
    line = lax.all_gather(right, "xy", axis=1, tiled=False)

    def turned(v, axis, step):
        n = lax.axis_size(axis)
        return lax.ppermute(v, axis, [((i + step) % n, i) for i in range(n)])

    def product(blocks, v):
        return jnp.einsum("dxjk,dxk->xj", blocks, v, precision=HIGHEST)

    def apply(v):
        near = [v, turned(v, "ta", 1), turned(v, "ta", -1), turned(v, "gz", 1), turned(v, "gz", -1)]
        near = jnp.stack(near + [jnp.roll(v, -1, 1), jnp.roll(v, 1, 1)], axis=1)
        re = product(split[0], near[0]) - product(split[1], near[1])
        im = product(split[0], near[1]) + product(split[1], near[0])
        return bottom_shift * v + jnp.stack([re, im])

    first = apply(line)
    second = apply(first)

    def inner(u, w):
        return [jnp.sum(u[0] * w[0] + u[1] * w[1]), jnp.sum(u[0] * w[1] - u[1] * w[0])]

    sums = inner(first, first)[:1] + inner(second, second)[:1] + inner(first, second)
    sums = sums + inner(first, line) + inner(second, line)
    ff, ss, cr, ci, pr, pi, qr, qi = lax.psum(jnp.stack(sums), ("ta", "gz"))
    det = ff * ss - cr * cr - ci * ci
    a_re = (ss * pr - (cr * qr - ci * qi)) / det
    a_im = (ss * pi - (cr * qi + ci * qr)) / det
    b_re = (ff * qr - (cr * pr + ci * pi)) / det
    b_im = (ff * qi - (cr * pi - ci * pr)) / det

    def scaled(re, im, v):
        return jnp.stack([re * v[0] - im * v[1], re * v[1] + im * v[0]])

    solved = scaled(a_re, a_im, line) + scaled(b_re, b_im, first)
    return lax.dynamic_index_in_dim(solved, lax.axis_index("xy"), 1, keepdims=False)


def shards(source_field, gauge_links, fine_vectors, middle_blocks, middle_vectors, bottom_blocks):
    axes = ("ta", "gz", "xy")
    shape = tuple(lax.axis_size(a) for a in axes)
    nt, nz, nx = shape
    devices = nt * nz * nx
    blocks = source_field.shape[-1] // BY
    source = source_field.reshape(SPINOR, LANES)
    gauge = gauge_links.reshape(-1, LANES)
    fine = jnp.transpose(fine_vectors, (0, 1, 3, 4, 5, 6, 2, 7)).reshape(-1, LANES)
    matrix = middle_blocks.reshape(-1, LANES)
    vectors = middle_vectors.reshape(-1, LANES)
    size = vectors.shape[0]
    project, rebuild = fine_tables()
    counts = [len(pairings(n)) for n in shape]
    gathered = nt == 4 and nz == 2 and 2 < nx and nx % 2 == 0 and nx * NVEC2 <= LANES

    halos = neighbours(source, axes)
    flat = [a for pair in halos for a in pair]
    loads = [source, gauge, fine, project, rebuild, vectors]
    shapes = [jax.ShapeDtypeStruct(a.shape, a.dtype) for a in loads]
    scratch = []
    depth = 0
    if gathered:
        depth = bottom_blocks.shape[-1] * 12 // LANES
        loads.append(bottom_blocks.reshape(1, -1))
        shapes.append(shape_of(depth, LANES))
        scratch.append(pltpu.VMEM(loads[-1].shape, F32))
    loaded = pl.pallas_call(
        functools.partial(load_kernel, gathered),
        out_shape=tuple(shapes),
        in_specs=[pl.BlockSpec(memory_space=pltpu.HBM)] * len(loads),
        out_specs=(vmem(),) * len(shapes),
        scratch_shapes=scratch + [pltpu.SemaphoreType.DMA((len(loads),))],
        compiler_params=params(4),
    )(*[pltpu.with_memory_space_constraint(a, pltpu.HBM) for a in loads])
    source, gauge, fine, project, rebuild, mine = loaded[:6]
    if gathered:
        line = loaded[6]
        beside = lax.ppermute(line, "ta", [(i, i ^ 1) for i in range(nt)])
        pair = jnp.concatenate([line, beside])
    spinor, payload = pl.pallas_call(
        functools.partial(first_kernel, counts, axes),
        out_shape=(shape_of(SPINOR, LANES), shape_of(SPINOR + size, LANES)),
        in_specs=[vmem()] * (len(flat) + 5),
        out_specs=(vmem(), vmem()),
        compiler_params=params(8),
    )(source, *flat, gauge, mine, project, rebuild)

    alone = (("ta", 0), ("xy", 1)) if gathered else ()
    near = neighbours(lambda axis, i: spinor if (axis, i) in alone else payload, axes)
    flat_near = [a for pair in near for a in pair]
    near_vectors = list(flat_near)
    if gathered:
        other = lax.ppermute(pair, "ta", [(i, i ^ 2) for i in range(nt)])
        near_vectors[0] = lax.ppermute(vectors, "ta", pairings(nt)[0])
        near_vectors[-1] = lax.ppermute(vectors, "xy", pairings(nx)[1])
    dests = devices if gathered else SUB
    residual, middle, sent = pl.pallas_call(
        functools.partial(second_kernel, counts, axes, blocks, gathered),
        out_shape=(
            shape_of(SPINOR, LANES),
            shape_of(2 * NVEC, LANES),
            shape_of(dests, LANES),
        ),
        in_specs=[vmem()] * (7 + len(flat_near)),
        out_specs=(vmem(), vmem(), vmem()),
        scratch_shapes=[pltpu.VMEM(fine.shape, F32)],
        compiler_params=params(8),
    )(source, spinor, *flat_near, gauge, fine, mine, project, rebuild)

    if gathered:
        received = lax.all_to_all(sent.reshape(devices, 1, LANES), axes, 0, 0)
        received = received.reshape(devices, LANES)
        received, pair, other = lax.optimization_barrier((received, pair, other))
        held = jnp.concatenate([pair, other])
        held = [held, lax.ppermute(held, "gz", pairings(nz)[0])]
        lane = np.arange(nx * NVEC2 * NVEC2)
        k_lane = np.arange(LANES)[:, None]
        spread = k_lane == (lane // (NVEC2 * NVEC2) * NVEC2 + lane % NVEC2)[None]
        gather = k_lane.T == (lane // NVEC2)[:, None]
        spread, gather = jnp.asarray(spread, BF16), jnp.asarray(gather, BF16)
        right, first_near, own = pl.pallas_call(
            functools.partial(start_kernel, shape),
            out_shape=(
                shape_of(2 * SUB, LANES),
                shape_of(6 * SUB, lane.size),
                shape_of(SUB, LANES),
            ),
            in_specs=[vmem()] * 4,
            out_specs=(vmem(),) * 3,
            scratch_shapes=[pltpu.VMEM((2 * SUB, lane.size), F32)],
            compiler_params=params(8),
        )(received, held[0], spread, gather)
        solution, residual = pl.pallas_call(
            functools.partial(third_kernel, counts, axes, blocks, shape),
            out_shape=(shape_of(SPINOR, LANES), shape_of(SPINOR, LANES)),
            in_specs=[vmem()] * (13 + len(flat_near)),
            out_specs=(vmem(), anywhere()),
            scratch_shapes=[
                pltpu.VMEM((6 * SUB, lane.size), F32),
                pltpu.VMEM((4 * SUB, lane.size), F32),
                pltpu.VMEM(fine.shape, F32),
                pltpu.SemaphoreType.DMA,
            ],
            compiler_params=params(8),
        )(right, residual, first_near, own, *held, spread, gather, matrix, mine, *near_vectors, middle, fine, spinor)
    else:
        solved = line_solve(sent[:2, :NVEC2], bottom_blocks)
        solved = jnp.pad(solved, ((0, 0), (0, LANES - NVEC2)))
        rows = [solved] + [a for pair in neighbours(solved, axes) for a in pair]
        rows = jnp.concatenate(rows)
        rows = jnp.pad(rows, ((0, 2 * SUB - rows.shape[0]), (0, 0)))
        solution = pl.pallas_call(
            functools.partial(fourth_kernel, counts, axes, blocks),
            out_shape=shape_of(SPINOR, LANES),
            in_specs=[vmem()] * (6 + len(flat_near)),
            out_specs=vmem(),
            scratch_shapes=[pltpu.VMEM(fine.shape, F32)],
            compiler_params=params(16),
        )(rows, matrix, mine, *near_vectors, middle, fine, spinor)
    return solution.reshape(source_field.shape), residual.reshape(source_field.shape)


def solution(mesh):
    return jax.shard_map(
        shards,
        mesh=mesh,
        in_specs=(
            P(None, None, None, "ta", "gz", "xy", None),
            P(None, None, None, None, "ta", "gz", "xy", None),
            P(None, None, None, None, "ta", "gz", "xy", None),
            P(None, None, None, "ta", "gz", "xy", None),
            P(None, None, "ta", "gz", "xy", None),
            P(None, None, "ta", "gz", None),
        ),
        out_specs=(
            P(None, None, None, "ta", "gz", "xy", None),
            P(None, None, None, "ta", "gz", "xy", None),
        ),
        check_vma=False,
    )
```
